32 devices in a mesh: gx: 4 (over x, core), gy: 8 (over z, y).
Axes of the slice: x: 2, y: 2, z: 4, core: 2. Of those that a mesh axis runs over, the one named last changes fastest.
Arguments:
- fine_source: bfloat16 [4, 8, 4, 8000], P('gx', 'gy'), may hold values from -6 to 6
- fine_blocks: bfloat16 [3, 12, 20, 20], replicated, may hold values from -0.5 to 0.5
- coarse_blocks: bfloat16 [3, 12, 20, 20], replicated, may hold values from -0.5 to 0.5
- child_filter_matrices: bfloat16 [2, 20, 20], replicated, may hold values from -1 to 1
Outputs:
- fine_result: float32 [4, 8, 4, 8000], P('gx', 'gy')
The draws below stay inside these ranges and needn't reach their ends.
All inputs are finite; a program needn't handle non-finite values.
Results may differ from the reference program's by a relative error of at most 0.013.
Values may be sent and summed in bfloat16 or wider, within the bound.
A program may use at most 64 MiB of HBM per device.

```python
import jax
import jax.numpy as jnp
from jax import lax

K2 = 20
TERMS = 12
FZ = 4
NXF = 4
NYF = 8


def block_levels(key, extent, split, smallest, top_value):
    factor_of = 1.0
    for position, parts in split:
        draws = jax.random.uniform(jax.random.fold_in(jax.random.fold_in(key, 6), position), (parts,), jnp.float32, smallest / len(split), top_value / len(split))
        factor_of = factor_of * jnp.repeat(jnp.exp(draws), extent[position] // parts).reshape((-1,) + (1,) * (len(extent) - 1 - position))
    return factor_of


def bell_draw(rng, extent, spread, most, cuts=(), kind=jnp.bfloat16):
    array = jax.random.normal(rng, extent, jnp.float32) * spread
    if len(cuts) > 0:
        array = block_levels(rng, extent, cuts, -0.22, 0.18) * array
    return jnp.clip(array, min=-most, max=most).astype(kind)


def setup_inputs(seed: int = 0) -> dict:
    keys = jax.random.split(jax.random.key(seed), 5)
    return {
        "fine_source": bell_draw(keys[0], (NXF, NYF, FZ, K2 * K2 * K2), 1.0, 6.0, ((0, 4), (1, 8))),
        "fine_blocks": bell_draw(keys[1], (3, TERMS, K2, K2), (6 * K2) ** -0.5, 0.5),
        "coarse_blocks": bell_draw(keys[2], (3, TERMS, K2, K2), (6 * K2) ** -0.5, 0.5),
        "child_filter_matrices": bell_draw(keys[3], (2, K2, K2), (2 * K2) ** -0.5, 1.0),
    }


def run_pass(values, matrix, coef_axis):
    matrix = matrix.astype(jnp.float32)
    values = values.astype(jnp.float32)
    if coef_axis == 0:
        return jnp.einsum('ca,...ajk->...cjk', matrix, values)
    if coef_axis == 1:
        return jnp.einsum('ca,...iak->...ick', matrix, values)
    return jnp.einsum('ca,...ija->...ijc', matrix, values)


def rounded(values):
    return lax.optimization_barrier(values.astype(jnp.bfloat16))


def shifted(values, grid_axis, offset):
    widths = [(0, 0)] * values.ndim
    widths[grid_axis] = (1, 1)
    padded = jnp.pad(values, widths)
    length = values.shape[grid_axis]
    return lax.slice_in_dim(padded, 1 + offset, 1 + offset + length, axis=grid_axis)


def apply_level(source, blocks):
    def one_term(summed, term_index):
        current = lax.dynamic_index_in_dim(blocks, term_index, 1, keepdims=False)
        lower_block, middle, upper_block = current[0], current[1], current[2]
        base_x = rounded(run_pass(source, middle, 0))
        upper_x = rounded(run_pass(shifted(source, 0, 1), upper_block, 0))
        lower_x = rounded(run_pass(shifted(source, 0, -1), lower_block, 0))
        base_y = rounded(run_pass(base_x, middle, 1))
        upper_y = rounded(run_pass(shifted(base_x, 1, 1), upper_block, 1))
        lower_child_y = rounded(run_pass(shifted(base_x, 1, -1), lower_block, 1))
        upper_xy = rounded(run_pass(upper_x, middle, 1))
        lower_xy = rounded(run_pass(lower_x, middle, 1))
        summed = summed + run_pass(base_y, middle, 2)
        summed = summed + run_pass(shifted(base_y, 2, 1), upper_block, 2)
        summed = summed + run_pass(shifted(base_y, 2, -1), lower_block, 2)
        summed = summed + run_pass(upper_y, middle, 2) + run_pass(lower_child_y, middle, 2)
        summed = summed + run_pass(upper_xy, middle, 2) + run_pass(lower_xy, middle, 2)
        return summed, None

    summed = jnp.zeros(source.shape, jnp.float32)
    summed, _ = lax.scan(one_term, summed, jnp.arange(TERMS, dtype=jnp.int32))
    return summed


def reference(fine_source, fine_blocks, coarse_blocks, child_filter_matrices):
    source = fine_source.reshape(NXF, NYF, FZ, K2, K2, K2)
    fine_term = apply_level(source, fine_blocks)
    scale_factors = child_filter_matrices.astype(jnp.float32)
    children = source.reshape(NXF // 2, 2, NYF // 2, 2, FZ // 2, 2, K2, K2, K2).astype(jnp.float32)
    after_x = rounded(jnp.einsum('ali,xaybzcijk->xaybzcljk', scale_factors, children)).astype(jnp.float32)
    after_y_pass = rounded(jnp.einsum('blj,xaybzcijk->xaybzcilk', scale_factors, after_x)).astype(jnp.float32)
    filtered_coefficients = jnp.einsum('fet,huwgofnmt->huwgofnme', scale_factors, after_y_pass)
    coarse_source = rounded(jnp.sum(filtered_coefficients, axis=(1, 3, 5)))
    coarse_result = rounded(apply_level(coarse_source, coarse_blocks)).astype(jnp.float32)
    grown_x = rounded(jnp.einsum('ail,xyzijk->xayzljk', scale_factors, coarse_result)).astype(jnp.float32)
    grown_y = rounded(jnp.einsum('bjm,xayzljk->xaybzlmk', scale_factors, grown_x)).astype(jnp.float32)
    expanded = jnp.einsum('ckn,xaybzlmk->xaybzclmn', scale_factors, grown_y)
    expanded = expanded.reshape(NXF, NYF, FZ, K2, K2, K2)
    return (fine_term + expanded).reshape(NXF, NYF, FZ, K2 * K2 * K2)
```

```python
import functools

import jax
import jax.numpy as jnp
from jax import lax
from jax.experimental import pallas as pl
from jax.experimental.pallas import tpu as pltpu
from jax.sharding import PartitionSpec as P

BF = jnp.bfloat16
F32 = jnp.float32
MESH = pl.DeviceIdType.MESH
ROW = 24
PAD = 32
LANES = 128
COLS = 5


def dot(a, b):
    return jnp.dot(a, b, preferred_element_type=F32)


def dot_t(a, b):
    return lax.dot_general(a, b, (((1,), (1,)), ((), ())), preferred_element_type=F32)


def grid2(rows, cols):
    r = lax.broadcasted_iota(jnp.int32, (rows, cols), 0)
    c = lax.broadcasted_iota(jnp.int32, (rows, cols), 1)
    return r, c


def one(cond):
    return jnp.where(cond, 1.0, 0.0).astype(BF)


def repeat_lanes(rows, period, valid):
    r, c = grid2(rows, LANES)
    return one((lax.rem(c, period) == r) & (c < valid))


def repeat_rows(cols, period, valid):
    r, c = grid2(LANES, cols)
    return one((lax.rem(r, period) == c) & (r < valid))


def pad_blocks(blk, pad, n):
    pad[...] = jnp.zeros_like(pad)
    for p in range(blk.shape[0]):
        pad[p * ROW : p * ROW + n, :n] = blk[p].astype(F32)


def three(pad, m, terms):
    return [pad[(e * terms + m) * ROW : (e * terms + m + 1) * ROW, :] for e in range(3)]


def build_first(pad, first, terms, grow):
    for m in range(terms):
        low, mid, up = three(pad, m, terms)
        rows = jnp.concatenate(
            [
                mid + pltpu.roll(up, ROW, 1) + pltpu.roll(low, 2 * ROW, 1),
                pltpu.roll(mid, 3 * ROW, 1),
                pltpu.roll(mid, 4 * ROW, 1),
                mid,
            ],
            axis=0,
        ).astype(BF)
        if grow is not None:
            rows = dot(grow, rows).astype(BF)
        first[m * 4 * ROW : (m + 1) * 4 * ROW, :] = rows


def widen(source, spread, wide, out, n, count, lanes):
    wide[: source.shape[0], :lanes] = dot(source, spread)
    r, c = grid2(16, lanes)
    keep = lax.rem(c, 8) == lax.rem(r, 8)

    def body(m, carry):
        base = pl.multiple_of(m * ROW, 8)
        block = wide[pl.ds(base, ROW), :lanes]
        for i in range(0, n, 2):
            pair = jnp.concatenate(
                [jnp.broadcast_to(block[i + h : i + h + 1, :], (8, lanes)) for h in range(2)], axis=0
            )
            out[m, i * 8 : (i + 2) * 8, :lanes] = jnp.where(keep, pair, 0.0).astype(BF)
        return carry

    if count == 1:
        body(0, 0)
    else:
        lax.fori_loop(0, count, body, 0)


def spread_eight(n, lanes, groups):
    r, c = grid2(LANES, lanes)
    n8 = n * 8
    return one((r == lax.div(c, n8) * PAD + lax.div(lax.rem(c, n8), 8)) & (c < groups * n8))


def build_second(pad, second, wide, terms, n, grow):
    cats = []
    for m in range(terms):
        low, mid, up = three(pad, m, terms)
        cats.append((mid + pltpu.roll(up, PAD, 1) + pltpu.roll(low, 2 * PAD, 1)).astype(BF))
    if grow is not None:
        cats = [
            dot(grow, jnp.concatenate(cats[m : m + 4], axis=0)).astype(BF) for m in range(0, terms, 4)
        ]
    source = jnp.concatenate(cats, axis=0)
    widen(source, spread_eight(n, 4 * LANES, 3), wide, second, n, terms, 4 * LANES)


def build_third(pad, third, terms, boxes, n, grow):
    valid = boxes * n
    wide = dot(pad[:, :PAD].astype(BF), repeat_lanes(PAD, n, valid)).astype(BF)
    left = repeat_rows(ROW, n, valid)
    r, c = grid2(LANES, LANES)
    row, col = lax.div(r, n), lax.div(c, n)
    for m in range(terms):
        low, mid, up = (
            dot(left, wide[(e * terms + m) * ROW : (e * terms + m + 1) * ROW]) for e in range(3)
        )
        at = m * 2 * LANES
        tile = jnp.concatenate(
            [
                jnp.where(row == col, mid, 0.0),
                jnp.where(col == row + 1, up, 0.0) + jnp.where(col == row - 1, low, 0.0),
            ],
            axis=1,
        ).astype(BF)
        if grow is not None:
            tile = dot(grow, tile).astype(BF)
        third[:, at : at + 2 * LANES] = tile


def pair_mats(mats, boxes_in, boxes_out, n):
    r, c = grid2(LANES, LANES)
    row, col = lax.div(r, n), lax.div(c, n)
    fine, parent = (col, row) if boxes_in > boxes_out else (row, col)
    keep = (lax.div(fine, 2) == parent) & (r < boxes_out * n) & (c < boxes_in * n)
    left = repeat_rows(PAD, n, boxes_out * n)
    right = repeat_lanes(PAD, n, boxes_in * n)
    tiles = [dot(left, dot(mats[e], right).astype(BF)) for e in range(2)]
    return jnp.where(keep, jnp.where(lax.rem(fine, 2) == 0, tiles[0], tiles[1]), 0.0).astype(BF)


def first_pass(u5, first, a, n, terms):
    def body(p, carry):
        rhs = jnp.concatenate([u5[2 * p], u5[2 * p + 1]], axis=1)
        o = dot(first[...], rhs)
        at = pl.multiple_of(p * 16, 16)
        for t in range(terms * 12):
            a[t, pl.ds(at, 16), :] = jnp.concatenate(
                [o[t * 8 : t * 8 + 8, :LANES], o[t * 8 : t * 8 + 8, LANES:]], axis=0
            ).astype(BF)
        return carry

    lax.fori_loop(0, n // 2, body, 0, unroll=5 if n % 10 == 0 else 1)


def second_pass(a, second, mid, n, terms):
    n8 = n * 8

    def body(m, carry):
        def field(f):
            return jnp.concatenate([a[(m * 4 + f) * 3 + g] for g in range(3)], axis=1)

        w = second[m]
        p = dot(w[:, : 3 * n8], jnp.concatenate([field(0), field(1), field(2)], axis=0)).astype(BF)
        q = dot(w[:, :n8], field(3)).astype(BF)
        for g in range(3):
            mid[m, g * n8 : (g + 1) * n8, :LANES] = p[:, g * LANES : (g + 1) * LANES]
            mid[m, g * n8 : (g + 1) * n8, LANES:] = q[:, g * LANES : (g + 1) * LANES]
        return carry

    lax.fori_loop(0, terms, body, 0, unroll=4 if terms % 4 == 0 else 1)


def third_pass(mid, third, terms):
    return dot_t(jnp.concatenate([mid[m] for m in range(terms)], axis=1), third[...])


def kernel(
    own,
    fine_blk,
    coarse_blk,
    filt,
    out,
    u5,
    c5,
    part,
    got,
    fpad,
    tpad,
    pad,
    wide,
    first,
    second,
    third,
    fsecond,
    fa,
    a,
    mid,
    fsend,
    frecv,
    psend,
    precv,
    csend,
    crecv,
    *,
    boxes,
    nx,
    ny,
):
    n = own.shape[0]
    n8 = n * 8
    terms = fine_blk.shape[0] // 3
    x, y = lax.axis_index("gx"), lax.axis_index("gy")
    px, py = lax.rem(x, 2), lax.rem(y, 2)
    mx, my = x + 1 - 2 * px, y + 1 - 2 * py

    near = [(x, y + 1, y < ny - 1), (x, y - 1, y > 0), (x + 1, y, x < nx - 1), (x - 1, y, x > 0)]
    far = [(x, y + 2, y < ny - 2), (x, y - 2, y > 1), (x + 2, y, x < nx - 2), (x - 2, y, x > 1)]
    mates = [(mx, y), (x, my), (mx, my)]
    back = [1, 0, 3, 2]

    def slot(c):
        return slice((c + 1) * ROW, (c + 2) * ROW)

    def near_copy(c):
        dx, dy, _ = near[c]
        b = back[c]
        return pltpu.make_async_remote_copy(
            src_ref=own,
            dst_ref=u5.at[:, slot(b), :],
            send_sem=fsend.at[c],
            recv_sem=frecv.at[b],
            device_id=(dx, dy),
            device_id_type=MESH,
        )

    def far_copy(c):
        dx, dy, _ = far[c]
        b = back[c]
        return pltpu.make_async_remote_copy(
            src_ref=c5.at[:, 0:ROW, :],
            dst_ref=c5.at[:, slot(b), :],
            send_sem=csend.at[c],
            recv_sem=crecv.at[b],
            device_id=(dx, dy),
            device_id_type=MESH,
        )

    def mate_copy(c):
        return pltpu.make_async_remote_copy(
            src_ref=part,
            dst_ref=got.at[c],
            send_sem=psend.at[c],
            recv_sem=precv.at[c],
            device_id=mates[c],
            device_id_type=MESH,
        )

    barrier = pltpu.get_barrier_semaphore()
    count = jnp.int32(1)
    pl.semaphore_signal(barrier, inc=1, device_id=mates[2], device_id_type=MESH)
    for dx, dy, exists in near + far:
        count = count + jnp.where(exists, 1, 0)

        @pl.when(exists)
        def _():
            pl.semaphore_signal(barrier, inc=1, device_id=(dx, dy), device_id_type=MESH)

    u5[:, 0:ROW, :] = own[...]
    for buf in (u5, c5):
        buf[:, COLS * ROW :, :] = jnp.zeros((n, LANES - COLS * ROW, LANES), BF)
    for group, buf in ((near, u5), (far, c5)):
        for c in range(4):

            @pl.when(jnp.logical_not(group[c][2]))
            def _():
                buf[:, slot(c), :] = jnp.zeros((n, ROW, LANES), BF)

    fpad[...] = jnp.zeros_like(fpad)
    for e in range(2):
        fpad[e, :n, :n] = filt[:, e, :].astype(F32)
    r, c = grid2(PAD, PAD)
    eye = one(r == c)
    mats = [fpad[e][:, :PAD].astype(BF) for e in range(2)]
    tpad[...] = jnp.zeros_like(tpad)
    for e in range(2):
        tpad[e, :, :PAD] = dot_t(eye, mats[e])
    turned = [tpad[e][:, :PAD].astype(BF) for e in range(2)]
    fy = fpad[py][:ROW, :ROW].astype(BF)
    fx = fpad[px][:ROW, :].astype(BF)
    widen(fx, spread_eight(n, 2 * LANES, 1), wide, fsecond, n, 1, 2 * LANES)
    fz = pair_mats(mats, boxes, boxes // 2, n)

    pl.semaphore_wait(barrier, count)
    for c in range(4):

        @pl.when(near[c][2])
        def _():
            near_copy(c).start()

    for p in range(n // 2):
        o = dot(fy, jnp.concatenate([own[2 * p], own[2 * p + 1]], axis=1))
        for g in range(3):
            fa[g, p * 16 : (p + 1) * 16, :] = jnp.concatenate(
                [o[g * 8 : g * 8 + 8, :LANES], o[g * 8 : g * 8 + 8, LANES:]], axis=0
            ).astype(BF)
    o = dot(fsecond[0][:, :n8], jnp.concatenate([fa[g] for g in range(3)], axis=1)).astype(BF)
    for g in range(3):
        s = dot_t(o[:, g * LANES : (g + 1) * LANES], fz)
        part[:, g * 8 : (g + 1) * 8, :] = s.reshape(n, 8, LANES).astype(BF)
    for c in range(3):
        mate_copy(c).start()

    pad_blocks(fine_blk, pad, n)
    build_first(pad, first, terms, None)
    build_second(pad, second, wide, terms, n, None)
    build_third(pad, third, terms, boxes, n, None)

    for c in range(3):
        mate_copy(c).wait_recv()
    total = part[...].astype(F32)
    for c in range(3):
        total = total + got[c].astype(F32)
    c5[:, 0:ROW, :] = total.astype(BF)
    for c in range(4):

        @pl.when(far[c][2])
        def _():
            far_copy(c).start()

    for c in range(4):

        @pl.when(near[c][2])
        def _():
            near_copy(back[c]).wait_recv()

    first_pass(u5, first, a, n, terms)
    second_pass(a, second, mid, n, terms)
    o = third_pass(mid, third, terms)
    for g in range(3):
        out[:, g * 8 : (g + 1) * 8, :] = o[g * n8 : (g + 1) * n8].reshape(n, 8, LANES)

    pad_blocks(coarse_blk, pad, n)
    r, c = grid2(4 * ROW, 4 * ROW)
    same = lax.div(r, ROW) == lax.div(c, ROW)
    rows4 = one(lax.rem(grid2(4 * ROW, PAD)[0], ROW) == grid2(4 * ROW, PAD)[1])
    cols4 = one(lax.rem(grid2(PAD, 4 * ROW)[1], ROW) == grid2(PAD, 4 * ROW)[0])

    def quad(mat):
        return jnp.where(same, dot(rows4, dot(mat, cols4).astype(BF)), 0.0).astype(BF)

    build_first(pad, first, terms, quad(tpad[py][:, :PAD].astype(BF)))
    build_second(pad, second, wide, terms, n, quad(tpad[px][:, :PAD].astype(BF)))
    build_third(pad, third, terms, boxes // 2, n, pair_mats(turned, boxes // 2, boxes, n))

    for c in range(4):

        @pl.when(far[c][2])
        def _():
            far_copy(back[c]).wait_recv()

    first_pass(c5, first, a, n, terms)
    second_pass(a, second, mid, n, terms)
    o = third_pass(mid, third, terms)
    for g in range(3):
        at = slice(g * 8, (g + 1) * 8)
        out[:, at, :] = out[:, at, :] + o[g * n8 : (g + 1) * n8].reshape(n, 8, LANES)

    for c in range(3):
        mate_copy(c).wait_send()
    for c in range(4):

        @pl.when(near[c][2])
        def _():
            near_copy(c).wait_send()

        @pl.when(far[c][2])
        def _():
            far_copy(c).wait_send()


VM = pl.BlockSpec(memory_space=pltpu.VMEM)


def shards(nx, ny, fine_source, fine_blocks, coarse_blocks, filters):
    boxes = fine_source.shape[2]
    terms, n = fine_blocks.shape[1], fine_blocks.shape[2]
    n8 = n * 8
    raw = fine_source.reshape(boxes, n, n, n)
    own = raw.transpose(1, 2, 0, 3).reshape(n, n, boxes * n)
    own = jnp.pad(own, ((0, 0), (0, ROW - n), (0, LANES - boxes * n)))
    dma = pltpu.SemaphoreType.DMA
    out = pl.pallas_call(
        functools.partial(kernel, boxes=boxes, nx=nx, ny=ny),
        out_shape=jax.ShapeDtypeStruct((n, ROW, LANES), F32),
        in_specs=[VM] * 4,
        out_specs=VM,
        scratch_shapes=[
            pltpu.VMEM((n, LANES, LANES), BF),
            pltpu.VMEM((n, LANES, LANES), BF),
            pltpu.VMEM((n, ROW, LANES), BF),
            pltpu.VMEM((3, n, ROW, LANES), BF),
            pltpu.VMEM((2, PAD, LANES), F32),
            pltpu.VMEM((2, PAD, LANES), F32),
            pltpu.VMEM((3 * terms * ROW, LANES), F32),
            pltpu.VMEM((terms * ROW, 4 * LANES), F32),
            pltpu.VMEM((terms * 4 * ROW, LANES), BF),
            pltpu.VMEM((terms, n8, 4 * LANES), BF),
            pltpu.VMEM((LANES, terms * 2 * LANES), BF),
            pltpu.VMEM((1, n8, 2 * LANES), BF),
            pltpu.VMEM((3, n8, LANES), BF),
            pltpu.VMEM((terms * 12, n8, LANES), BF),
            pltpu.VMEM((terms, 3 * n8, 2 * LANES), BF),
            dma((4,)),
            dma((4,)),
            dma((3,)),
            dma((3,)),
            dma((4,)),
            dma((4,)),
        ],
        compiler_params=pltpu.CompilerParams(
            vmem_limit_bytes=60 * 1024 * 1024, collective_id=0, has_side_effects=True
        ),
    )(
        own,
        fine_blocks.reshape(3 * terms, n, n),
        coarse_blocks.reshape(3 * terms, n, n),
        filters.transpose(1, 0, 2),
    )
    out = out[:, :n, : boxes * n].reshape(n, n, boxes, n).transpose(2, 0, 1, 3)
    return out.reshape(1, 1, boxes, n * n * n)


def solution(mesh):
    in_specs = (P("gx", "gy", None, None), P(), P(), P())
    out_specs = P("gx", "gy", None, None)
    body = functools.partial(shards, mesh.shape["gx"], mesh.shape["gy"])
    return jax.shard_map(body, mesh=mesh, in_specs=in_specs, out_specs=out_specs, check_vma=False)
```

```python
import functools

import jax
import jax.numpy as jnp
from jax import lax
from jax.experimental import pallas as pl
from jax.experimental.pallas import tpu as pltpu
from jax.sharding import PartitionSpec as P

BF = jnp.bfloat16
F32 = jnp.float32
MESH = pl.DeviceIdType.MESH
ROW = 24
PAD = 32
LANES = 128


def dot(a, b):
    return jnp.dot(a, b, preferred_element_type=F32)


def dot_t(a, b):
    return lax.dot_general(a, b, (((1,), (1,)), ((), ())), preferred_element_type=F32)


def grid2(rows, cols):
    r = lax.broadcasted_iota(jnp.int32, (rows, cols), 0)
    c = lax.broadcasted_iota(jnp.int32, (rows, cols), 1)
    return r, c


def one(cond):
    return jnp.where(cond, 1.0, 0.0).astype(BF)


def repeat_lanes(rows, period, valid):
    r, c = grid2(rows, LANES)
    return one((lax.rem(c, period) == r) & (c < valid))


def repeat_rows(cols, period, valid):
    r, c = grid2(LANES, cols)
    return one((lax.rem(r, period) == c) & (r < valid))


def cats(blk, pad, n, terms):
    pad[...] = jnp.zeros_like(pad)
    for p in range(3 * terms):
        pad[p * ROW : p * ROW + n, :n] = blk[p].astype(F32)


def three(pad, m, terms):
    return [pad[(e * terms + m) * ROW : (e * terms + m + 1) * ROW, :] for e in range(3)]


def build_first(pad, first, terms):
    for m in range(terms):
        low, mid, up = three(pad, m, terms)
        first[m * ROW : (m + 1) * ROW, :] = (
            mid + pltpu.roll(up, ROW, 1) + pltpu.roll(low, 2 * ROW, 1)
        ).astype(BF)


def grown(first, mat, terms):
    step = mat.shape[0]
    rows = [dot(mat, first[m : m + step, :]).astype(BF) for m in range(0, terms * ROW, step)]
    return jnp.concatenate(rows, axis=0)


def widen(source, spread, wide, out, n, count, lanes):
    wide[: source.shape[0], :lanes] = dot(source, spread)
    r, c = grid2(16, lanes)
    keep = lax.rem(c, 8) == lax.rem(r, 8)

    def body(m, carry):
        base = pl.multiple_of(m * ROW, 8)
        block = wide[pl.ds(base, ROW), :lanes]
        for i in range(0, n, 2):
            pair = jnp.concatenate(
                [jnp.broadcast_to(block[i + h : i + h + 1, :], (8, lanes)) for h in range(2)], axis=0
            )
            out[m, i * 8 : (i + 2) * 8, :lanes] = jnp.where(keep, pair, 0.0).astype(BF)
        return carry

    if count == 1:
        body(0, 0)
    else:
        lax.fori_loop(0, count, body, 0)


def spread_eight(n, lanes, groups):
    r, c = grid2(LANES, lanes)
    n8 = n * 8
    return one((r == lax.div(c, n8) * ROW + lax.div(lax.rem(c, n8), 8)) & (c < groups * n8))


def build_second(source, second, wide, terms, n):
    widen(source, spread_eight(n, 4 * LANES, 3), wide, second, n, terms, 4 * LANES)


def build_third(pad, third, terms, boxes, n, grow):
    both = grow is not None
    wide = dot(pad[:, :PAD].astype(BF), repeat_lanes(PAD, n, boxes * n * (1 + both))).astype(BF)
    left = repeat_rows(ROW, n, boxes * n)
    r, c = grid2(LANES, LANES)
    row, col = lax.div(r, n), lax.div(c, n)
    side = col - boxes if both else col
    for m in range(terms):
        low, mid, up = (
            dot(left, wide[(e * terms + m) * ROW : (e * terms + m + 1) * ROW]) for e in range(3)
        )
        main = jnp.where((row == col) & (col < boxes), mid, 0.0)
        other = jnp.where(side == row + 1, up, 0.0)
        other = other + jnp.where((side == row - 1) & (side >= 0), low, 0.0)
        if both:
            third[:, m * LANES : (m + 1) * LANES] = dot(grow, (main + other).astype(BF)).astype(BF)
        else:
            at = m * 2 * LANES
            third[:, at : at + LANES] = main.astype(BF)
            third[:, at + LANES : at + 2 * LANES] = other.astype(BF)


def pair_mats(mats, boxes_in, boxes_out, n):
    r, c = grid2(LANES, LANES)
    row, col = lax.div(r, n), lax.div(c, n)
    fine, parent = (col, row) if boxes_in > boxes_out else (row, col)
    keep = (lax.div(fine, 2) == parent) & (r < boxes_out * n) & (c < boxes_in * n)
    left = repeat_rows(PAD, n, boxes_out * n)
    right = repeat_lanes(PAD, n, boxes_in * n)
    tiles = [dot(left, dot(mats[e], right).astype(BF)) for e in range(2)]
    return jnp.where(keep, jnp.where(lax.rem(fine, 2) == 0, tiles[0], tiles[1]), 0.0)


def lane(shape):
    return lax.broadcasted_iota(jnp.int32, shape, 1)


def pack(src, dst, n, kappa):
    at = lane((ROW, LANES))
    for q in range((n + 2) // 3):
        tile = [src[3 * q + h].astype(F32) if 3 * q + h < n else None for h in range(3)]
        r1 = pltpu.roll(tile[1], kappa, 1)
        dst[2 * q] = jnp.where(at < kappa, tile[0], r1).astype(BF)
        r2 = jnp.zeros_like(r1) if tile[2] is None else pltpu.roll(tile[2], 2 * kappa - LANES, 1)
        dst[2 * q + 1] = jnp.where(at < 2 * kappa - LANES, r1, r2).astype(BF)


def unpack(src, dst, rows, n, kappa):
    at = lane((ROW, LANES))
    for q in range((n + 2) // 3):
        a, b = src[2 * q].astype(F32), src[2 * q + 1].astype(F32)
        dst[3 * q, rows, :] = a.astype(BF)
        dst[3 * q + 1, rows, :] = pltpu.roll(jnp.where(at >= kappa, a, b), LANES - kappa, 1).astype(BF)
        if 3 * q + 2 < n:
            dst[3 * q + 2, rows, :] = pltpu.roll(b, 2 * (LANES - kappa), 1).astype(BF)


def unpack_parent(src, dst, rows, n, kappa, twice):
    at = lane((ROW, LANES))
    deep = (n + 2) // 3
    for s in range(deep):
        tile = src[s].astype(F32)
        for t in range(3):
            if t * deep + s < n:
                v = tile if t == 0 else pltpu.roll(tile, LANES - t * kappa, 1)
                other = 0.0
                if twice:
                    other = tile if t == 1 else pltpu.roll(tile, (LANES - (t - 1) * kappa) % LANES, 1)
                dst[t * deep + s, rows, :] = jnp.where(at < kappa, v, other).astype(BF)


def first_pass(u, rows, w, a, n, blocks):
    def body(p, carry):
        rhs = jnp.concatenate([u[2 * p, :rows, :], u[2 * p + 1, :rows, :]], axis=1)
        o = dot(w[:, :rows], rhs)
        at = pl.multiple_of(p * 16, 16)
        for t in range(blocks):
            a[t, pl.ds(at, 16), :] = jnp.concatenate(
                [o[t * 8 : t * 8 + 8, :LANES], o[t * 8 : t * 8 + 8, LANES:]], axis=0
            ).astype(BF)
        return carry

    lax.fori_loop(0, n // 2, body, 0, unroll=5 if n % 10 == 0 else 1)


def second_pass(fields, second, mid, n, terms, at):
    n8 = n * 8
    k = len(fields) * n8

    def body(m, carry):
        rhs = jnp.concatenate(
            [jnp.concatenate([a[m * 3 + g] for g in range(3)], axis=1) for a in fields], axis=0
        )
        p = dot(second[m][:, :k], rhs).astype(BF)
        for g in range(3):
            mid[m, g * n8 : (g + 1) * n8, at : at + LANES] = p[:, g * LANES : (g + 1) * LANES]
        return carry

    lax.fori_loop(0, terms, body, 0, unroll=4 if terms % 4 == 0 else 1)


def third_pass(mid, third, terms):
    return dot_t(jnp.concatenate([mid[m] for m in range(terms)], axis=1), third[...])


def kernel(
    own,
    fine_blk,
    coarse_blk,
    filt,
    out,
    opk,
    npk,
    u,
    ux,
    part,
    half,
    got,
    cpk,
    ppk,
    cu,
    cx,
    fpad,
    tpad,
    pad,
    wide,
    first,
    second,
    third,
    first_c,
    second_c,
    third_c,
    fsecond,
    fa,
    a,
    mid,
    mid_c,
    fsend,
    frecv,
    psend,
    precv,
    csend,
    crecv,
    *,
    boxes,
    nx,
    ny,
):
    n = own.shape[0]
    n8 = n * 8
    terms = fine_blk.shape[0] // 3
    kappa = boxes * n
    half_k = kappa // 2
    deep = (n + 2) // 3
    x, y = lax.axis_index("gx"), lax.axis_index("gy")
    px, py = lax.rem(x, 2), lax.rem(y, 2)
    mates = [(x + 1 - 2 * px, y), (x, y + 1 - 2 * py)]
    near = [(x, y + 1, y < ny - 1), (x, y - 1, y > 0), (x + 1, y, x < nx - 1), (x - 1, y, x > 0)]
    far = [(x, y + 2, y < ny - 2), (x, y - 2, y > 1), (x + 2, y, x < nx - 2), (x - 2, y, x > 1)]
    back = [1, 0, 3, 2]

    def near_copy(c):
        b = back[c]
        return pltpu.make_async_remote_copy(
            src_ref=opk.at[:, :n, :],
            dst_ref=npk.at[b, :, :n, :],
            send_sem=fsend.at[c],
            recv_sem=frecv.at[b],
            device_id=near[c][:2],
            device_id_type=MESH,
        )

    def far_copy(c):
        b = back[c]
        return pltpu.make_async_remote_copy(
            src_ref=cpk.at[:, :n, :],
            dst_ref=ppk.at[b, :, :n, :],
            send_sem=csend.at[c],
            recv_sem=crecv.at[b],
            device_id=far[c][:2],
            device_id_type=MESH,
        )

    def mate_copy(c):
        return pltpu.make_async_remote_copy(
            src_ref=(part, half)[c].at[:, :n, :],
            dst_ref=got.at[c, :, :n, :],
            send_sem=psend.at[c],
            recv_sem=precv.at[c],
            device_id=mates[c],
            device_id_type=MESH,
        )

    barrier = pltpu.get_barrier_semaphore()
    count = jnp.int32(0)
    for dx, dy, exists in near + far:
        count = count + jnp.where(exists, 1, 0)

        @pl.when(exists)
        def _():
            pl.semaphore_signal(barrier, inc=1, device_id=(dx, dy), device_id_type=MESH)

    for c in range(4):
        npk[c, :, n:, :] = jnp.zeros((2 * deep, ROW - n, LANES), BF)
        ppk[c, :, n:, :] = jnp.zeros((deep, ROW - n, LANES), BF)

        @pl.when(jnp.logical_not(near[c][2]))
        def _():
            npk[c, :, :n, :] = jnp.zeros((2 * deep, n, LANES), BF)

        @pl.when(jnp.logical_not(far[c][2]))
        def _():
            ppk[c, :, :n, :] = jnp.zeros((deep, n, LANES), BF)

    pack(own, opk, n, kappa)

    fpad[...] = jnp.zeros_like(fpad)
    for e in range(2):
        fpad[e, :n, :n] = filt[:, e, :].astype(F32)
    r, c = grid2(PAD, PAD)
    eye = one(r == c)
    mats = [fpad[e][:, :PAD].astype(BF) for e in range(2)]
    tpad[...] = jnp.zeros_like(tpad)
    for e in range(2):
        tpad[e, :, :PAD] = dot_t(eye, mats[e])
    turned = [tpad[e][:, :PAD].astype(BF) for e in range(2)]
    fy = fpad[py][:ROW, :ROW].astype(BF)
    fx = fpad[px][:ROW, :].astype(BF)
    widen(fx, spread_eight(n, 2 * LANES, 1), wide, fsecond, n, 1, 2 * LANES)
    fz = pair_mats(mats, boxes, boxes // 2, n)
    turns = [fz if t == 0 else pltpu.roll(fz, t * half_k, 0) for t in range(3)]
    fz3 = jnp.concatenate(turns, axis=1).astype(BF)

    pl.semaphore_wait(barrier, count)
    for c in (2, 3, 0, 1):

        @pl.when(near[c][2])
        def _():
            near_copy(c).start()

    for p in range(n // 2):
        o = dot(fy, jnp.concatenate([own[2 * p], own[2 * p + 1]], axis=1))
        for g in range(3):
            fa[g, p * 16 : (p + 1) * 16, :] = jnp.concatenate(
                [o[g * 8 : g * 8 + 8, :LANES], o[g * 8 : g * 8 + 8, LANES:]], axis=0
            ).astype(BF)
    o = dot(fsecond[0][:, :n8], jnp.concatenate([fa[g] for g in range(3)], axis=1))
    o = jnp.concatenate([o, jnp.zeros(((3 * deep - n) * 8, 3 * LANES), F32)], axis=0).astype(BF)
    d8 = deep * 8
    for g in range(3):
        s = dot_t(
            jnp.concatenate(
                [o[t * d8 : (t + 1) * d8, g * LANES : (g + 1) * LANES] for t in range(3)], axis=1
            ),
            fz3,
        )
        part[:, g * 8 : (g + 1) * 8, :] = s.reshape(deep, 8, LANES).astype(BF)
    mate_copy(0).start()

    cats(fine_blk, pad, n, terms)
    build_first(pad, first, terms)
    build_second(first[...], second, wide, terms, n)

    mate_copy(0).wait_recv()
    half[:, :n, :] = (part[:, :n, :].astype(F32) + got[0, :, :n, :].astype(F32)).astype(BF)
    mate_copy(1).start()

    build_third(pad, third, terms, boxes, n, None)
    first_pass(own, ROW, first, a.at[3], n, terms * 3)
    second_pass([a.at[3]], second, mid, n, terms, LANES)

    mate_copy(1).wait_recv()
    cpk[:, n:, :] = jnp.zeros((deep, ROW - n, LANES), BF)
    cpk[:, :n, :] = (half[:, :n, :].astype(F32) + got[1, :, :n, :].astype(F32)).astype(BF)
    for c in range(4):

        @pl.when(far[c][2])
        def _():
            far_copy(c).start()

    cats(coarse_blk, pad, n, terms)
    build_first(pad, first_c, terms)
    r, c = grid2(4 * ROW, 4 * ROW)
    same = lax.div(r, ROW) == lax.div(c, ROW)
    rows4 = one(lax.rem(grid2(4 * ROW, PAD)[0], ROW) == grid2(4 * ROW, PAD)[1])
    cols4 = one(lax.rem(grid2(PAD, 4 * ROW)[1], ROW) == grid2(PAD, 4 * ROW)[0])

    def quad(mat):
        return jnp.where(same, dot(rows4, dot(mat, cols4).astype(BF)), 0.0).astype(BF)

    build_second(grown(first_c, quad(tpad[px][:, :PAD].astype(BF)), terms), second_c, wide, terms, n)
    first_c[...] = grown(first_c, quad(tpad[py][:, :PAD].astype(BF)), terms)
    build_third(pad, third_c, terms, boxes // 2, n, pair_mats(turned, boxes // 2, boxes, n).astype(BF))

    def near_wait(c):
        @pl.when(near[c][2])
        def _():
            near_copy(back[c]).wait_recv()

    for c in (2, 3):
        near_wait(c)
        unpack(npk.at[c], ux.at[c - 2], slice(0, ROW), n, kappa)
        first_pass(ux.at[c - 2], ROW, first, a.at[c - 1], n, terms * 3)
    u[:, :ROW, :] = own[...]
    for c in (0, 1):
        near_wait(c)
        unpack(npk.at[c], u, slice((c + 1) * ROW, (c + 2) * ROW), n, kappa)
    first_pass(u, 3 * ROW, first, a.at[0], n, terms * 3)
    second_pass([a.at[0], a.at[1], a.at[2]], second, mid, n, terms, 0)
    o = third_pass(mid, third, terms)
    for g in range(3):
        out[:, g * 8 : (g + 1) * 8, :] = o[g * n8 : (g + 1) * n8].reshape(n, 8, LANES)

    unpack_parent(cpk, cu, slice(0, ROW), n, half_k, True)
    for c in range(4):

        @pl.when(far[c][2])
        def _():
            far_copy(back[c]).wait_recv()

        if c < 2:
            unpack_parent(ppk.at[c], cu, slice((c + 1) * ROW, (c + 2) * ROW), n, half_k, False)
        else:
            unpack_parent(ppk.at[c], cx.at[c - 2], slice(0, ROW), n, half_k, False)
    first_pass(cx.at[0], ROW, first_c, a.at[1], n, terms * 3)
    first_pass(cx.at[1], ROW, first_c, a.at[2], n, terms * 3)
    first_pass(cu, 3 * ROW, first_c, a.at[0], n, terms * 3)
    second_pass([a.at[0], a.at[1], a.at[2]], second_c, mid_c, n, terms, 0)
    o = third_pass(mid_c, third_c, terms)
    for g in range(3):
        at = slice(g * 8, (g + 1) * 8)
        out[:, at, :] = out[:, at, :] + o[g * n8 : (g + 1) * n8].reshape(n, 8, LANES)

    for c in range(2):
        mate_copy(c).wait_send()
    for c in range(4):

        @pl.when(near[c][2])
        def _():
            near_copy(c).wait_send()

        @pl.when(far[c][2])
        def _():
            far_copy(c).wait_send()


VM = pl.BlockSpec(memory_space=pltpu.VMEM)


def shards(nx, ny, fine_source, fine_blocks, coarse_blocks, filters):
    boxes = fine_source.shape[2]
    terms, n = fine_blocks.shape[1], fine_blocks.shape[2]
    n8 = n * 8
    deep = (n + 2) // 3
    raw = fine_source.reshape(boxes, n, n, n)
    own = raw.transpose(1, 2, 0, 3).reshape(n, n, boxes * n)
    own = jnp.pad(own, ((0, 0), (0, ROW - n), (0, LANES - boxes * n)))
    dma = pltpu.SemaphoreType.DMA

    def bf(*shape):
        return pltpu.VMEM(shape, BF)

    def f32(*shape):
        return pltpu.VMEM(shape, F32)

    out = pl.pallas_call(
        functools.partial(kernel, boxes=boxes, nx=nx, ny=ny),
        out_shape=jax.ShapeDtypeStruct((n, ROW, LANES), F32),
        in_specs=[VM] * 4,
        out_specs=VM,
        scratch_shapes=[
            bf(2 * deep, ROW, LANES),
            bf(4, 2 * deep, ROW, LANES),
            bf(n, 3 * ROW, LANES),
            bf(2, n, ROW, LANES),
            bf(deep, ROW, LANES),
            bf(deep, ROW, LANES),
            bf(2, deep, ROW, LANES),
            bf(deep, ROW, LANES),
            bf(4, deep, ROW, LANES),
            bf(n, 3 * ROW, LANES),
            bf(2, n, ROW, LANES),
            f32(2, PAD, LANES),
            f32(2, PAD, LANES),
            f32(3 * terms * ROW, LANES),
            f32(terms * ROW, 4 * LANES),
            bf(terms * ROW, LANES),
            bf(terms, n8, 4 * LANES),
            bf(LANES, terms * 2 * LANES),
            bf(terms * ROW, LANES),
            bf(terms, n8, 4 * LANES),
            bf(LANES, terms * LANES),
            bf(1, n8, 2 * LANES),
            bf(3, n8, LANES),
            bf(4, terms * 3, n8, LANES),
            bf(terms, 3 * n8, 2 * LANES),
            bf(terms, 3 * n8, LANES),
            dma((4,)),
            dma((4,)),
            dma((2,)),
            dma((2,)),
            dma((4,)),
            dma((4,)),
        ],
        compiler_params=pltpu.CompilerParams(
            vmem_limit_bytes=60 * 1024 * 1024, collective_id=0, has_side_effects=True
        ),
    )(
        own,
        fine_blocks.reshape(3 * terms, n, n),
        coarse_blocks.reshape(3 * terms, n, n),
        filters.transpose(1, 0, 2),
    )
    out = out[:, :n, : boxes * n].reshape(n, n, boxes, n).transpose(2, 0, 1, 3)
    return out.reshape(1, 1, boxes, n * n * n)


def solution(mesh):
    in_specs = (P("gx", "gy", None, None), P(), P(), P())
    out_specs = P("gx", "gy", None, None)
    body = functools.partial(shards, mesh.shape["gx"], mesh.shape["gy"])
    return jax.shard_map(body, mesh=mesh, in_specs=in_specs, out_specs=out_specs, check_vma=False)
```

```python
import functools

import jax
import jax.numpy as jnp
from jax import lax
from jax.experimental import pallas as pl
from jax.experimental.pallas import tpu as pltpu
from jax.sharding import PartitionSpec as P

BF = jnp.bfloat16
F32 = jnp.float32
MESH = pl.DeviceIdType.MESH
ROW = 24
PAD = 32
LANES = 128


def dot(a, b):
    return jnp.dot(a, b, preferred_element_type=F32)


def dot_t(a, b):
    return lax.dot_general(a, b, (((1,), (1,)), ((), ())), preferred_element_type=F32)


def grid2(rows, cols):
    r = lax.broadcasted_iota(jnp.int32, (rows, cols), 0)
    c = lax.broadcasted_iota(jnp.int32, (rows, cols), 1)
    return r, c


def one(cond):
    return jnp.where(cond, 1.0, 0.0).astype(BF)


def repeat_lanes(rows, period, valid):
    r, c = grid2(rows, LANES)
    return one((lax.rem(c, period) == r) & (c < valid))


def repeat_rows(cols, period, valid):
    r, c = grid2(LANES, cols)
    return one((lax.rem(r, period) == c) & (r < valid))


def cats(blk, pad, n, terms):
    pad[...] = jnp.zeros_like(pad)
    for p in range(3 * terms):
        pad[p * ROW : p * ROW + n, :n] = blk[p].astype(F32)


def three(pad, m, terms):
    return [pad[(e * terms + m) * ROW : (e * terms + m + 1) * ROW, :] for e in range(3)]


def build_first(pad, first, terms):
    for m in range(terms):
        low, mid, up = three(pad, m, terms)
        first[m * ROW : (m + 1) * ROW, :] = (
            mid + pltpu.roll(up, ROW, 1) + pltpu.roll(low, 2 * ROW, 1)
        ).astype(BF)


def grown(first, mat, terms):
    step = mat.shape[0]
    rows = [dot(mat, first[m : m + step, :]).astype(BF) for m in range(0, terms * ROW, step)]
    return jnp.concatenate(rows, axis=0)


def widen(source, spread, wide, out, n, count, lanes):
    wide[: source.shape[0], :lanes] = dot(source, spread)
    r, c = grid2(16, lanes)
    keep = lax.rem(c, 8) == lax.rem(r, 8)

    def body(m, carry):
        base = pl.multiple_of(m * ROW, 8)
        block = wide[pl.ds(base, ROW), :lanes]
        for i in range(0, n, 2):
            pair = jnp.concatenate(
                [jnp.broadcast_to(block[i + h : i + h + 1, :], (8, lanes)) for h in range(2)], axis=0
            )
            out[m, i * 8 : (i + 2) * 8, :lanes] = jnp.where(keep, pair, 0.0).astype(BF)
        return carry

    if count == 1:
        body(0, 0)
    else:
        lax.fori_loop(0, count, body, 0, unroll=2)


def spread_eight(n, lanes, groups):
    r, c = grid2(LANES, lanes)
    n8 = n * 8
    return one((r == lax.div(c, n8) * ROW + lax.div(lax.rem(c, n8), 8)) & (c < groups * n8))


def build_second(source, second, wide, terms, n):
    widen(source, spread_eight(n, 4 * LANES, 3), wide, second, n, terms, 4 * LANES)


def build_third(pad, third, terms, boxes, n, grow):
    both = grow is not None
    wide = dot(pad[:, :PAD].astype(BF), repeat_lanes(PAD, n, boxes * n * (1 + both))).astype(BF)
    left = repeat_rows(ROW, n, boxes * n)
    r, c = grid2(LANES, LANES)
    row, col = lax.div(r, n), lax.div(c, n)
    side = col - boxes if both else col
    for m in range(terms):
        low, mid, up = (
            dot(left, wide[(e * terms + m) * ROW : (e * terms + m + 1) * ROW]) for e in range(3)
        )
        main = jnp.where((row == col) & (col < boxes), mid, 0.0)
        other = jnp.where(side == row + 1, up, 0.0)
        other = other + jnp.where((side == row - 1) & (side >= 0), low, 0.0)
        if both:
            third[:, m * LANES : (m + 1) * LANES] = dot(grow, (main + other).astype(BF)).astype(BF)
        else:
            at = m * 2 * LANES
            third[:, at : at + LANES] = main.astype(BF)
            third[:, at + LANES : at + 2 * LANES] = other.astype(BF)


def pair_mats(mats, boxes_in, boxes_out, n):
    r, c = grid2(LANES, LANES)
    row, col = lax.div(r, n), lax.div(c, n)
    fine, parent = (col, row) if boxes_in > boxes_out else (row, col)
    keep = (lax.div(fine, 2) == parent) & (r < boxes_out * n) & (c < boxes_in * n)
    left = repeat_rows(PAD, n, boxes_out * n)
    right = repeat_lanes(PAD, n, boxes_in * n)
    tiles = [dot(left, dot(mats[e], right).astype(BF)) for e in range(2)]
    return jnp.where(keep, jnp.where(lax.rem(fine, 2) == 0, tiles[0], tiles[1]), 0.0)


def lane(shape):
    return lax.broadcasted_iota(jnp.int32, shape, 1)


def pack(src, dst, n, kappa):
    at = lane((ROW, LANES))
    for q in range((n + 2) // 3):
        tile = [src[3 * q + h].astype(F32) if 3 * q + h < n else None for h in range(3)]
        r1 = pltpu.roll(tile[1], kappa, 1)
        dst[2 * q] = jnp.where(at < kappa, tile[0], r1).astype(BF)
        r2 = jnp.zeros_like(r1) if tile[2] is None else pltpu.roll(tile[2], 2 * kappa - LANES, 1)
        dst[2 * q + 1] = jnp.where(at < 2 * kappa - LANES, r1, r2).astype(BF)


def unpack(src, dst, rows, n, kappa):
    at = lane((ROW, LANES))
    for q in range((n + 2) // 3):
        a, b = src[2 * q].astype(F32), src[2 * q + 1].astype(F32)
        dst[3 * q, rows, :] = a.astype(BF)
        dst[3 * q + 1, rows, :] = pltpu.roll(jnp.where(at >= kappa, a, b), LANES - kappa, 1).astype(BF)
        if 3 * q + 2 < n:
            dst[3 * q + 2, rows, :] = pltpu.roll(b, 2 * (LANES - kappa), 1).astype(BF)


def unpack_parent(src, dst, rows, n, kappa, twice):
    at = lane((ROW, LANES))
    deep = (n + 2) // 3
    for s in range(deep):
        tile = src[s].astype(F32)
        for t in range(3):
            if t * deep + s < n:
                v = tile if t == 0 else pltpu.roll(tile, LANES - t * kappa, 1)
                other = 0.0
                if twice:
                    other = tile if t == 1 else pltpu.roll(tile, (LANES - (t - 1) * kappa) % LANES, 1)
                dst[t * deep + s, rows, :] = jnp.where(at < kappa, v, other).astype(BF)


def tiles_of(base, rows, n):
    return base // LANES, (base + rows * n - 1) // LANES


def mirror(n):
    r, c = grid2(LANES, LANES)
    group, p = lax.div(c, ROW), lax.rem(c, ROW)
    g, s = lax.div(p, 8), lax.rem(p, 8)
    count = jnp.minimum(n - 8 * g, 8)
    return one((s < count) & (r == group * ROW + 8 * g + count - 1 - s) & (group < 3))


def skew(v, n):
    v = pltpu.roll(v, 0, 1, stride=n // 2, stride_axis=0)
    return pltpu.roll(v, 0, 1, stride=n - n // 2, stride_axis=0)


def unflatten(raw, flat, own, boxes, n):
    size = raw.shape[-1]
    flat[:, size // LANES * LANES :] = jnp.zeros((boxes, flat.shape[1] - size // LANES * LANES), F32)
    flat[:, :size] = raw[0, 0].astype(F32)
    s, at = grid2(8, LANES)
    offset = at + s * n
    place = lax.rem(at + s * n, LANES)
    below = [place < (z + 1) * n for z in range(boxes)]
    for i in range(n):
        rows = []
        for g in range(ROW // 8):
            base = (i * n + 8 * g + min(8, n - 8 * g) - 1) * n
            t = (base - 7 * n) // LANES
            c = base - t * LANES
            v = None
            for z in reversed(range(boxes)):

                def tile(k):
                    line = flat[z : z + 1, (t + k) * LANES : (t + k + 1) * LANES]
                    return jnp.broadcast_to(line, (8, LANES))

                w = jnp.where(offset >= c, tile(0), tile(1))
                if c + n > 2 * LANES:
                    w = jnp.where(offset >= c - LANES, w, tile(2))
                w = pltpu.roll(w, (z * n - c) % LANES, 1)
                v = w if v is None else jnp.where(below[z], w, v)
            rows.append(skew(v, n))
        own[i] = jnp.concatenate(rows, axis=0).astype(BF)


def flatten(rows, out, boxes, n):
    size = out.shape[-1]
    s, at = grid2(8, LANES)
    offset = at - s * n
    total = [[None] * (-(-size // LANES)) for _ in range(boxes)]
    for i in range(n):
        for g in range(ROW // 8):
            base = (i * n + 8 * g) * n
            count = min(8, n - 8 * g)
            first, last = base // LANES, (base + count * n - 1) // LANES
            c = base - first * LANES
            v = skew(rows(g, i), n)
            turned = [pltpu.roll(v, (c - z * n) % LANES, 1) for z in range(boxes)]
            for t in range(first, last + 1):
                lo = c - (t - first) * LANES
                keep = (offset >= lo) & (offset < lo + n)
                if count < 8:
                    keep = keep & (s < count)
                for z in range(boxes):
                    old = total[z][t]
                    total[z][t] = jnp.where(keep, turned[z], 0.0 if old is None else old)
        for t in range(len(total[0])):
            if total[0][t] is not None and ((t + 1) * LANES <= (i + 1) * n * n or i == n - 1):
                end = min((t + 1) * LANES, size)
                for z in range(boxes):
                    line = jnp.sum(total[z][t], axis=0, keepdims=True)
                    out[0, 0, z : z + 1, t * LANES : end] = line[:, : end - t * LANES]
                    total[z][t] = None


def first_pass(u, rows, w, a, n, blocks):
    def body(p, carry):
        rhs = jnp.concatenate([u[2 * p, :rows, :], u[2 * p + 1, :rows, :]], axis=1)
        o = dot(w[:, :rows], rhs)
        at = pl.multiple_of(p * 16, 16)
        for t in range(blocks):
            a[t, pl.ds(at, 16), :] = jnp.concatenate(
                [o[t * 8 : t * 8 + 8, :LANES], o[t * 8 : t * 8 + 8, LANES:]], axis=0
            ).astype(BF)
        return carry

    lax.fori_loop(0, n // 2, body, 0, unroll=True)


def second_pass(fields, second, mid, n, terms, at):
    n8 = n * 8
    k = len(fields) * n8

    def body(m, carry):
        rhs = jnp.concatenate(
            [jnp.concatenate([a[m * 3 + g] for g in range(3)], axis=1) for a in fields], axis=0
        )
        p = dot(second[m][:, :k], rhs).astype(BF)
        for g in range(3):
            mid[m, g * n8 : (g + 1) * n8, at : at + LANES] = p[:, g * LANES : (g + 1) * LANES]
        return carry

    lax.fori_loop(0, terms, body, 0, unroll=True)


def third_pass(mid, third, terms):
    return dot_t(jnp.concatenate([mid[m] for m in range(terms)], axis=1), third[...])


def kernel(
    raw_hbm,
    fine_hbm,
    coarse_hbm,
    filt_hbm,
    out,
    raw,
    filt,
    own,
    flat,
    fine_blk,
    coarse_blk,
    acc,
    opk,
    npk,
    u,
    ux,
    part,
    half,
    got,
    cpk,
    ppk,
    cu,
    cx,
    fpad,
    tpad,
    pad,
    wide,
    first,
    second,
    third,
    first_c,
    second_c,
    third_c,
    fsecond,
    fa,
    a,
    mid,
    mid_c,
    fsend,
    frecv,
    psend,
    precv,
    csend,
    crecv,
    bsem,
    *,
    boxes,
    nx,
    ny,
):
    n = own.shape[0]
    n8 = n * 8
    terms = fine_blk.shape[0] // 3
    kappa = boxes * n
    half_k = kappa // 2
    deep = (n + 2) // 3
    x, y = lax.axis_index("gx"), lax.axis_index("gy")
    px, py = lax.rem(x, 2), lax.rem(y, 2)
    mates = [(x + 1 - 2 * px, y), (x, y + 1 - 2 * py)]
    near = [(x, y + 1, y < ny - 1), (x, y - 1, y > 0), (x + 1, y, x < nx - 1), (x - 1, y, x > 0)]
    far = [(x, y + 2, y < ny - 2), (x, y - 2, y > 1), (x + 2, y, x < nx - 2), (x - 2, y, x > 1)]
    back = [1, 0, 3, 2]

    def near_copy(c):
        b = back[c]
        return pltpu.make_async_remote_copy(
            src_ref=opk.at[:, :n, :],
            dst_ref=npk.at[b, :, :n, :],
            send_sem=fsend.at[c],
            recv_sem=frecv.at[b],
            device_id=near[c][:2],
            device_id_type=MESH,
        )

    def far_copy(c):
        b = back[c]
        return pltpu.make_async_remote_copy(
            src_ref=cpk.at[:, :n, :],
            dst_ref=ppk.at[b, :, :n, :],
            send_sem=csend.at[c],
            recv_sem=crecv.at[b],
            device_id=far[c][:2],
            device_id_type=MESH,
        )

    def mate_copy(c):
        return pltpu.make_async_remote_copy(
            src_ref=(part, half)[c].at[:, :n, :],
            dst_ref=got.at[c, :, :n, :],
            send_sem=psend.at[c],
            recv_sem=precv.at[c],
            device_id=mates[c],
            device_id_type=MESH,
        )

    fetch = [
        pltpu.make_async_copy(raw_hbm, raw, bsem.at[2]),
        pltpu.make_async_copy(filt_hbm, filt, bsem.at[3]),
        pltpu.make_async_copy(fine_hbm, fine_blk, bsem.at[0]),
        pltpu.make_async_copy(coarse_hbm, coarse_blk, bsem.at[1]),
    ]
    for f in fetch:
        f.start()
    barrier = pltpu.get_barrier_semaphore()
    count = jnp.int32(0)
    for dx, dy, exists in near + far:
        count = count + jnp.where(exists, 1, 0)

        @pl.when(exists)
        def _():
            pl.semaphore_signal(barrier, inc=1, device_id=(dx, dy), device_id_type=MESH)

    for c in range(4):
        npk[c, :, n:, :] = jnp.zeros((2 * deep, ROW - n, LANES), BF)
        ppk[c, :, n:, :] = jnp.zeros((deep, ROW - n, LANES), BF)

        @pl.when(jnp.logical_not(near[c][2]))
        def _():
            npk[c, :, :n, :] = jnp.zeros((2 * deep, n, LANES), BF)

        @pl.when(jnp.logical_not(far[c][2]))
        def _():
            ppk[c, :, :n, :] = jnp.zeros((deep, n, LANES), BF)

    fetch[0].wait()
    unflatten(raw, flat, own, boxes, n)
    pack(own, opk, n, kappa)

    fpad[...] = jnp.zeros_like(fpad)
    fetch[1].wait()
    for e in range(2):
        fpad[e, :n, :n] = filt[:, e, :].astype(F32)
    r, c = grid2(PAD, PAD)
    eye = one(r == c)
    mats = [fpad[e][:, :PAD].astype(BF) for e in range(2)]
    tpad[...] = jnp.zeros_like(tpad)
    for e in range(2):
        tpad[e, :, :PAD] = dot_t(eye, mats[e])
    turned = [tpad[e][:, :PAD].astype(BF) for e in range(2)]
    perm = mirror(n)
    fy = dot(fpad[py][:ROW, :].astype(BF), perm)[:, :ROW].astype(BF)
    fx = fpad[px][:ROW, :].astype(BF)
    widen(fx, spread_eight(n, 2 * LANES, 1), wide, fsecond, n, 1, 2 * LANES)
    fz = pair_mats(mats, boxes, boxes // 2, n)
    turns = [fz if t == 0 else pltpu.roll(fz, t * half_k, 0) for t in range(3)]
    fz3 = jnp.concatenate(turns, axis=1).astype(BF)

    pl.semaphore_wait(barrier, count)
    for c in (2, 3, 0, 1):

        @pl.when(near[c][2])
        def _():
            near_copy(c).start()

    for p in range(n // 2):
        o = dot(fy, jnp.concatenate([own[2 * p], own[2 * p + 1]], axis=1))
        for g in range(3):
            fa[g, p * 16 : (p + 1) * 16, :] = jnp.concatenate(
                [o[g * 8 : g * 8 + 8, :LANES], o[g * 8 : g * 8 + 8, LANES:]], axis=0
            ).astype(BF)
    o = dot(fsecond[0][:, :n8], jnp.concatenate([fa[g] for g in range(3)], axis=1))
    o = jnp.concatenate([o, jnp.zeros(((3 * deep - n) * 8, 3 * LANES), F32)], axis=0).astype(BF)
    d8 = deep * 8
    for g in range(3):
        s = dot_t(
            jnp.concatenate(
                [o[t * d8 : (t + 1) * d8, g * LANES : (g + 1) * LANES] for t in range(3)], axis=1
            ),
            fz3,
        )
        part[:, g * 8 : (g + 1) * 8, :] = s.reshape(deep, 8, LANES).astype(BF)
    mate_copy(0).start()

    fetch[2].wait()
    cats(fine_blk, pad, n, terms)
    build_first(pad, first, terms)
    build_second(first[...], second, wide, terms, n)
    first[...] = dot(first[...], perm).astype(BF)

    mate_copy(0).wait_recv()
    half[:, :n, :] = (part[:, :n, :].astype(F32) + got[0, :, :n, :].astype(F32)).astype(BF)
    mate_copy(1).start()

    build_third(pad, third, terms, boxes, n, None)
    first_pass(own, ROW, first, a.at[3], n, terms * 3)
    second_pass([a.at[3]], second, mid, n, terms, LANES)

    mate_copy(1).wait_recv()
    cpk[:, n:, :] = jnp.zeros((deep, ROW - n, LANES), BF)
    cpk[:, :n, :] = (half[:, :n, :].astype(F32) + got[1, :, :n, :].astype(F32)).astype(BF)
    for c in range(4):

        @pl.when(far[c][2])
        def _():
            far_copy(c).start()

    fetch[3].wait()
    cats(coarse_blk, pad, n, terms)
    build_first(pad, first_c, terms)
    r, c = grid2(4 * ROW, 4 * ROW)
    same = lax.div(r, ROW) == lax.div(c, ROW)
    rows4 = one(lax.rem(grid2(4 * ROW, PAD)[0], ROW) == grid2(4 * ROW, PAD)[1])
    cols4 = one(lax.rem(grid2(PAD, 4 * ROW)[1], ROW) == grid2(PAD, 4 * ROW)[0])

    def quad(mat):
        return jnp.where(same, dot(rows4, dot(mat, cols4).astype(BF)), 0.0).astype(BF)

    build_second(grown(first_c, quad(tpad[px][:, :PAD].astype(BF)), terms), second_c, wide, terms, n)
    first_c[...] = grown(first_c, quad(tpad[py][:, :PAD].astype(BF)), terms)
    build_third(pad, third_c, terms, boxes // 2, n, pair_mats(turned, boxes // 2, boxes, n).astype(BF))

    def near_wait(c):
        @pl.when(near[c][2])
        def _():
            near_copy(back[c]).wait_recv()

    for c in (2, 3):
        near_wait(c)
        unpack(npk.at[c], ux.at[c - 2], slice(0, ROW), n, kappa)
        first_pass(ux.at[c - 2], ROW, first, a.at[c - 1], n, terms * 3)
    u[:, :ROW, :] = own[...]
    for c in (0, 1):
        near_wait(c)
        unpack(npk.at[c], u, slice((c + 1) * ROW, (c + 2) * ROW), n, kappa)
    first_pass(u, 3 * ROW, first, a.at[0], n, terms * 3)
    second_pass([a.at[0], a.at[1], a.at[2]], second, mid, n, terms, 0)
    acc[...] = third_pass(mid, third, terms)

    unpack_parent(cpk, cu, slice(0, ROW), n, half_k, True)
    for c in range(4):

        @pl.when(far[c][2])
        def _():
            far_copy(back[c]).wait_recv()

        if c < 2:
            unpack_parent(ppk.at[c], cu, slice((c + 1) * ROW, (c + 2) * ROW), n, half_k, False)
        else:
            unpack_parent(ppk.at[c], cx.at[c - 2], slice(0, ROW), n, half_k, False)
    first_pass(cx.at[0], ROW, first_c, a.at[1], n, terms * 3)
    first_pass(cx.at[1], ROW, first_c, a.at[2], n, terms * 3)
    first_pass(cu, 3 * ROW, first_c, a.at[0], n, terms * 3)
    second_pass([a.at[0], a.at[1], a.at[2]], second_c, mid_c, n, terms, 0)
    acc[...] += third_pass(mid_c, third_c, terms)
    flatten(lambda g, i: acc[g * n8 + i * 8 : g * n8 + (i + 1) * 8, :], out, boxes, n)

    for c in range(2):
        mate_copy(c).wait_send()
    for c in range(4):

        @pl.when(near[c][2])
        def _():
            near_copy(c).wait_send()

        @pl.when(far[c][2])
        def _():
            far_copy(c).wait_send()


VM = pl.BlockSpec(memory_space=pltpu.VMEM)


def in_hbm(x):
    return pltpu.with_memory_space_constraint(x, pltpu.HBM)


def shards(nx, ny, fine_source, fine_blocks, coarse_blocks, filters):
    boxes = fine_source.shape[2]
    terms, n = fine_blocks.shape[1], fine_blocks.shape[2]
    n8 = n * 8
    deep = (n + 2) // 3
    dma = pltpu.SemaphoreType.DMA

    def bf(*shape):
        return pltpu.VMEM(shape, BF)

    def f32(*shape):
        return pltpu.VMEM(shape, F32)

    return pl.pallas_call(
        functools.partial(kernel, boxes=boxes, nx=nx, ny=ny),
        out_shape=jax.ShapeDtypeStruct(fine_source.shape, F32),
        in_specs=[pl.BlockSpec(memory_space=pltpu.HBM)] * 4,
        out_specs=VM,
        scratch_shapes=[
            bf(*fine_source.shape),
            bf(n, 2, n),
            bf(n, ROW, LANES),
            f32(boxes, (fine_source.shape[3] // LANES + 3) * LANES),
            bf(3 * terms, n, n),
            bf(3 * terms, n, n),
            f32(3 * n8, LANES),
            bf(2 * deep, ROW, LANES),
            bf(4, 2 * deep, ROW, LANES),
            bf(n, 3 * ROW, LANES),
            bf(2, n, ROW, LANES),
            bf(deep, ROW, LANES),
            bf(deep, ROW, LANES),
            bf(2, deep, ROW, LANES),
            bf(deep, ROW, LANES),
            bf(4, deep, ROW, LANES),
            bf(n, 3 * ROW, LANES),
            bf(2, n, ROW, LANES),
            f32(2, PAD, LANES),
            f32(2, PAD, LANES),
            f32(3 * terms * ROW, LANES),
            f32(terms * ROW, 4 * LANES),
            bf(terms * ROW, LANES),
            bf(terms, n8, 4 * LANES),
            bf(LANES, terms * 2 * LANES),
            bf(terms * ROW, LANES),
            bf(terms, n8, 4 * LANES),
            bf(LANES, terms * LANES),
            bf(1, n8, 2 * LANES),
            bf(3, n8, LANES),
            bf(4, terms * 3, n8, LANES),
            bf(terms, 3 * n8, 2 * LANES),
            bf(terms, 3 * n8, LANES),
            dma((4,)),
            dma((4,)),
            dma((2,)),
            dma((2,)),
            dma((4,)),
            dma((4,)),
            dma((4,)),
        ],
        compiler_params=pltpu.CompilerParams(
            vmem_limit_bytes=32 * 1024 * 1024, collective_id=0, has_side_effects=True
        ),
    )(
        in_hbm(fine_source),
        in_hbm(fine_blocks.reshape(3 * terms, n, n)),
        in_hbm(coarse_blocks.reshape(3 * terms, n, n)),
        in_hbm(filters.transpose(1, 0, 2)),
    )


def solution(mesh):
    in_specs = (P("gx", "gy", None, None), P(), P(), P())
    out_specs = P("gx", "gy", None, None)
    body = functools.partial(shards, mesh.shape["gx"], mesh.shape["gy"])
    return jax.shard_map(body, mesh=mesh, in_specs=in_specs, out_specs=out_specs, check_vma=False)
```

```python
import functools

import jax
import jax.numpy as jnp
from jax import lax
from jax.experimental import pallas as pl
from jax.experimental.pallas import tpu as pltpu
from jax.sharding import PartitionSpec as P

BF = jnp.bfloat16
F32 = jnp.float32
MESH = pl.DeviceIdType.MESH
ROW = 24
PAD = 32
LANES = 128


def dot(a, b):
    return jnp.dot(a, b, preferred_element_type=F32)


def dot_t(a, b):
    return lax.dot_general(a, b, (((1,), (1,)), ((), ())), preferred_element_type=F32)


def grid2(rows, cols):
    r = lax.broadcasted_iota(jnp.int32, (rows, cols), 0)
    c = lax.broadcasted_iota(jnp.int32, (rows, cols), 1)
    return r, c


def one(cond):
    return jnp.where(cond, 1.0, 0.0).astype(BF)


def repeat_lanes(rows, period, valid):
    r, c = grid2(rows, LANES)
    return one((lax.rem(c, period) == r) & (c < valid))


def repeat_rows(cols, period, valid):
    r, c = grid2(LANES, cols)
    return one((lax.rem(r, period) == c) & (r < valid))


def cats(blk, pad, n, terms):
    pad[...] = jnp.zeros_like(pad)
    for p in range(3 * terms):
        pad[p * ROW : p * ROW + n, :n] = blk[p].astype(F32)


def three(pad, m, terms):
    return [pad[(e * terms + m) * ROW : (e * terms + m + 1) * ROW, :] for e in range(3)]


def build_first(pad, first, terms):
    for m in range(terms):
        low, mid, up = three(pad, m, terms)
        first[m * ROW : (m + 1) * ROW, :] = (
            mid + pltpu.roll(up, ROW, 1) + pltpu.roll(low, 2 * ROW, 1)
        ).astype(BF)


def grown(first, mat, terms):
    step = mat.shape[0]
    rows = [dot(mat, first[m : m + step, :]).astype(BF) for m in range(0, terms * ROW, step)]
    return jnp.concatenate(rows, axis=0)


def widen(source, spread, wide, out, n, count, lanes):
    wide[: source.shape[0], :lanes] = dot(source, spread)
    r, c = grid2(16, lanes)
    keep = lax.rem(c, 8) == lax.rem(r, 8)

    def body(m, carry):
        base = pl.multiple_of(m * ROW, 8)
        block = wide[pl.ds(base, ROW), :lanes]
        for i in range(0, n, 2):
            pair = jnp.concatenate(
                [jnp.broadcast_to(block[i + h : i + h + 1, :], (8, lanes)) for h in range(2)], axis=0
            )
            out[m, i * 8 : (i + 2) * 8, :lanes] = jnp.where(keep, pair, 0.0).astype(BF)
        return carry

    if count == 1:
        body(0, 0)
    else:
        lax.fori_loop(0, count, body, 0, unroll=2)


def spread_eight(n, lanes, groups):
    r, c = grid2(LANES, lanes)
    n8 = n * 8
    return one((r == lax.div(c, n8) * ROW + lax.div(lax.rem(c, n8), 8)) & (c < groups * n8))


def build_second(source, second, wide, terms, n):
    widen(source, spread_eight(n, 4 * LANES, 3), wide, second, n, terms, 4 * LANES)


def build_third(pad, lines, third, terms, boxes, n, grow):
    both = grow is not None
    lines[...] = dot(pad[:, :PAD].astype(BF), repeat_lanes(PAD, n, boxes * n * (1 + both)))
    col = lax.div(grid2(ROW, LANES)[1], n)
    spare = jnp.zeros((LANES - boxes * ROW, LANES), F32)
    for m in range(terms):
        low, mid, up = three(lines, m, terms)
        main, other = [], []
        for z in range(boxes):
            shift = boxes if both else 0
            side = jnp.where(col == shift + z + 1, up, 0.0)
            if z > 0:
                side = jnp.where(col == shift + z - 1, low, side)
            if both:
                main.append(jnp.where(col == z, mid, side))
            else:
                main.append(jnp.where(col == z, mid, 0.0))
                other.append(side)
        if both:
            tile = jnp.concatenate(main, axis=0).astype(BF)
            third[:, m * LANES : (m + 1) * LANES] = dot(grow, tile).astype(BF)
        else:
            at = m * 2 * LANES
            third[:, at : at + LANES] = jnp.concatenate(main + [spare], axis=0).astype(BF)
            third[:, at + LANES : at + 2 * LANES] = jnp.concatenate(other + [spare], axis=0).astype(BF)


def growth(tpad, boxes):
    rows = [
        tpad[e][:ROW] if z == 0 else pltpu.roll(tpad[e][:ROW], z * ROW, 1)
        for z in range(boxes)
        for e in range(2)
    ]
    rows.append(jnp.zeros((LANES - 2 * boxes * ROW, LANES), F32))
    return jnp.concatenate(rows, axis=0).astype(BF)[:, : boxes * ROW]


def pair_mats(mats, boxes_in, boxes_out, n):
    r, c = grid2(LANES, LANES)
    row, col = lax.div(r, n), lax.div(c, n)
    fine, parent = (col, row) if boxes_in > boxes_out else (row, col)
    keep = (lax.div(fine, 2) == parent) & (r < boxes_out * n) & (c < boxes_in * n)
    left = repeat_rows(PAD, n, boxes_out * n)
    right = repeat_lanes(PAD, n, boxes_in * n)
    tiles = [dot(left, dot(mats[e], right).astype(BF)) for e in range(2)]
    return jnp.where(keep, jnp.where(lax.rem(fine, 2) == 0, tiles[0], tiles[1]), 0.0)


def lane(shape):
    return lax.broadcasted_iota(jnp.int32, shape, 1)


def pack(src, dst, n, kappa):
    at = lane((ROW, LANES))
    for q in range((n + 2) // 3):
        tile = [src[3 * q + h].astype(F32) if 3 * q + h < n else None for h in range(3)]
        r1 = pltpu.roll(tile[1], kappa, 1)
        dst[2 * q] = jnp.where(at < kappa, tile[0], r1).astype(BF)
        r2 = jnp.zeros_like(r1) if tile[2] is None else pltpu.roll(tile[2], 2 * kappa - LANES, 1)
        dst[2 * q + 1] = jnp.where(at < 2 * kappa - LANES, r1, r2).astype(BF)


def unpack(src, dst, rows, n, kappa):
    at = lane((ROW, LANES))
    for q in range((n + 2) // 3):
        a, b = src[2 * q].astype(F32), src[2 * q + 1].astype(F32)
        dst[3 * q, rows, :] = a.astype(BF)
        dst[3 * q + 1, rows, :] = pltpu.roll(jnp.where(at >= kappa, a, b), LANES - kappa, 1).astype(BF)
        if 3 * q + 2 < n:
            dst[3 * q + 2, rows, :] = pltpu.roll(b, 2 * (LANES - kappa), 1).astype(BF)


def unpack_parent(src, dst, rows, n, kappa, twice):
    at = lane((ROW, LANES))
    deep = (n + 2) // 3
    for s in range(deep):
        tile = src[s].astype(F32)
        for t in range(3):
            if t * deep + s < n:
                v = tile if t == 0 else pltpu.roll(tile, LANES - t * kappa, 1)
                other = 0.0
                if twice:
                    other = tile if t == 1 else pltpu.roll(tile, (LANES - (t - 1) * kappa) % LANES, 1)
                dst[t * deep + s, rows, :] = jnp.where(at < kappa, v, other).astype(BF)


def tiles_of(base, rows, n):
    return base // LANES, (base + rows * n - 1) // LANES


def mirror(n):
    r, c = grid2(LANES, LANES)
    group, p = lax.div(c, ROW), lax.rem(c, ROW)
    g, s = lax.div(p, 8), lax.rem(p, 8)
    count = jnp.minimum(n - 8 * g, 8)
    return one((s < count) & (r == group * ROW + 8 * g + count - 1 - s) & (group < 3))


def skew(v, n):
    v = pltpu.roll(v, 0, 1, stride=n // 2, stride_axis=0)
    return pltpu.roll(v, 0, 1, stride=n - n // 2, stride_axis=0)


def unflatten(raw, flat, own, boxes, n):
    size = raw.shape[-1]
    flat[:, size // LANES * LANES :] = jnp.zeros((boxes, flat.shape[1] - size // LANES * LANES), F32)
    flat[:, :size] = raw[0, 0].astype(F32)
    s, at = grid2(8, LANES)
    offset = at + s * n
    place = lax.rem(at + s * n, LANES)
    below = [place < (z + 1) * n for z in range(boxes)]
    for i in range(n):
        rows = []
        for g in range(ROW // 8):
            base = (i * n + 8 * g + min(8, n - 8 * g) - 1) * n
            t = (base - 7 * n) // LANES
            c = base - t * LANES
            v = None
            for z in reversed(range(boxes)):

                def tile(k):
                    line = flat[z : z + 1, (t + k) * LANES : (t + k + 1) * LANES]
                    return jnp.broadcast_to(line, (8, LANES))

                w = jnp.where(offset >= c, tile(0), tile(1))
                if c + n > 2 * LANES:
                    w = jnp.where(offset >= c - LANES, w, tile(2))
                w = pltpu.roll(w, (z * n - c) % LANES, 1)
                v = w if v is None else jnp.where(below[z], w, v)
            rows.append(skew(v, n))
        own[i] = jnp.concatenate(rows, axis=0).astype(BF)


def flatten(rows, out, boxes, n):
    size = out.shape[-1]
    s, at = grid2(8, LANES)
    offset = at - s * n
    total = [[None] * (-(-size // LANES)) for _ in range(boxes)]
    for i in range(n):
        for g in range(ROW // 8):
            base = (i * n + 8 * g) * n
            count = min(8, n - 8 * g)
            first, last = base // LANES, (base + count * n - 1) // LANES
            c = base - first * LANES
            v = skew(rows(g, i), n)
            turned = [pltpu.roll(v, (c - z * ROW) % LANES, 1) for z in range(boxes)]
            for t in range(first, last + 1):
                lo = c - (t - first) * LANES
                keep = (offset >= lo) & (offset < lo + n)
                if count < 8:
                    keep = keep & (s < count)
                for z in range(boxes):
                    old = total[z][t]
                    total[z][t] = jnp.where(keep, turned[z], 0.0 if old is None else old)
        for t in range(len(total[0])):
            if total[0][t] is not None and ((t + 1) * LANES <= (i + 1) * n * n or i == n - 1):
                end = min((t + 1) * LANES, size)
                for z in range(boxes):
                    line = jnp.sum(total[z][t], axis=0, keepdims=True)
                    out[0, 0, z : z + 1, t * LANES : end] = line[:, : end - t * LANES]
                    total[z][t] = None


def first_pass(u, rows, w, a, n, blocks):
    def body(p, carry):
        rhs = jnp.concatenate([u[2 * p, :rows, :], u[2 * p + 1, :rows, :]], axis=1)
        o = dot(w[:, :rows], rhs)
        at = pl.multiple_of(p * 16, 16)
        for t in range(blocks):
            a[t, pl.ds(at, 16), :] = jnp.concatenate(
                [o[t * 8 : t * 8 + 8, :LANES], o[t * 8 : t * 8 + 8, LANES:]], axis=0
            ).astype(BF)
        return carry

    lax.fori_loop(0, n // 2, body, 0, unroll=True)


def second_pass(fields, second, mid, n, terms, at):
    n8 = n * 8
    k = len(fields) * n8

    def body(m, carry):
        rhs = jnp.concatenate(
            [jnp.concatenate([a[m * 3 + g] for g in range(3)], axis=1) for a in fields], axis=0
        )
        p = dot(second[m][:, :k], rhs).astype(BF)
        for g in range(3):
            mid[m, g * n8 : (g + 1) * n8, at : at + LANES] = p[:, g * LANES : (g + 1) * LANES]
        return carry

    lax.fori_loop(0, terms, body, 0, unroll=True)


def third_pass(mid, third, terms):
    return dot_t(jnp.concatenate([mid[m] for m in range(terms)], axis=1), third[...])


def kernel(
    raw_hbm,
    fine_hbm,
    coarse_hbm,
    filt_hbm,
    out,
    raw,
    filt,
    own,
    flat,
    fine_blk,
    coarse_blk,
    acc,
    lines,
    opk,
    npk,
    u,
    ux,
    part,
    half,
    got,
    cpk,
    ppk,
    cu,
    cx,
    fpad,
    tpad,
    pad,
    wide,
    first,
    second,
    third,
    first_c,
    second_c,
    third_c,
    fsecond,
    fa,
    a,
    mid,
    mid_c,
    fsend,
    frecv,
    psend,
    precv,
    csend,
    crecv,
    bsem,
    *,
    boxes,
    nx,
    ny,
):
    n = own.shape[0]
    n8 = n * 8
    terms = fine_blk.shape[0] // 3
    kappa = boxes * n
    half_k = kappa // 2
    deep = (n + 2) // 3
    x, y = lax.axis_index("gx"), lax.axis_index("gy")
    px, py = lax.rem(x, 2), lax.rem(y, 2)
    mates = [(x + 1 - 2 * px, y), (x, y + 1 - 2 * py)]
    near = [(x, y + 1, y < ny - 1), (x, y - 1, y > 0), (x + 1, y, x < nx - 1), (x - 1, y, x > 0)]
    far = [(x, y + 2, y < ny - 2), (x, y - 2, y > 1), (x + 2, y, x < nx - 2), (x - 2, y, x > 1)]
    back = [1, 0, 3, 2]

    def near_copy(c):
        b = back[c]
        return pltpu.make_async_remote_copy(
            src_ref=opk.at[:, :n, :],
            dst_ref=npk.at[b, :, :n, :],
            send_sem=fsend.at[c],
            recv_sem=frecv.at[b],
            device_id=near[c][:2],
            device_id_type=MESH,
        )

    def far_copy(c):
        b = back[c]
        return pltpu.make_async_remote_copy(
            src_ref=cpk.at[:, :n, :],
            dst_ref=ppk.at[b, :, :n, :],
            send_sem=csend.at[c],
            recv_sem=crecv.at[b],
            device_id=far[c][:2],
            device_id_type=MESH,
        )

    def mate_copy(c):
        return pltpu.make_async_remote_copy(
            src_ref=(part, half)[c].at[:, :n, :],
            dst_ref=got.at[c, :, :n, :],
            send_sem=psend.at[c],
            recv_sem=precv.at[c],
            device_id=mates[c],
            device_id_type=MESH,
        )

    fetch = [
        pltpu.make_async_copy(raw_hbm, raw, bsem.at[2]),
        pltpu.make_async_copy(filt_hbm, filt, bsem.at[3]),
        pltpu.make_async_copy(fine_hbm, fine_blk, bsem.at[0]),
        pltpu.make_async_copy(coarse_hbm, coarse_blk, bsem.at[1]),
    ]
    for f in fetch:
        f.start()
    barrier = pltpu.get_barrier_semaphore()
    count = jnp.int32(0)
    for dx, dy, exists in near + far:
        count = count + jnp.where(exists, 1, 0)

        @pl.when(exists)
        def _():
            pl.semaphore_signal(barrier, inc=1, device_id=(dx, dy), device_id_type=MESH)

    for c in range(4):
        npk[c, :, n:, :] = jnp.zeros((2 * deep, ROW - n, LANES), BF)
        ppk[c, :, n:, :] = jnp.zeros((deep, ROW - n, LANES), BF)

        @pl.when(jnp.logical_not(near[c][2]))
        def _():
            npk[c, :, :n, :] = jnp.zeros((2 * deep, n, LANES), BF)

        @pl.when(jnp.logical_not(far[c][2]))
        def _():
            ppk[c, :, :n, :] = jnp.zeros((deep, n, LANES), BF)

    fetch[0].wait()
    fetch[1].wait()
    unflatten(raw, flat, own, boxes, n)
    pack(own, opk, n, kappa)

    fpad[...] = jnp.zeros_like(fpad)
    for e in range(2):
        fpad[e, :n, :n] = filt[:, e, :].astype(F32)
    r, c = grid2(PAD, PAD)
    eye = one(r == c)
    mats = [fpad[e][:, :PAD].astype(BF) for e in range(2)]
    tpad[...] = jnp.zeros_like(tpad)
    for e in range(2):
        tpad[e, :, :PAD] = dot_t(eye, mats[e])
    perm = mirror(n)
    fy = dot(fpad[py][:ROW, :].astype(BF), perm)[:, :ROW].astype(BF)
    fx = fpad[px][:ROW, :].astype(BF)
    widen(fx, spread_eight(n, 2 * LANES, 1), wide, fsecond, n, 1, 2 * LANES)
    fz = pair_mats(mats, boxes, boxes // 2, n)
    turns = [fz if t == 0 else pltpu.roll(fz, t * half_k, 0) for t in range(3)]
    fz3 = jnp.concatenate(turns, axis=1).astype(BF)

    pl.semaphore_wait(barrier, count)
    for c in (2, 3, 0, 1):

        @pl.when(near[c][2])
        def _():
            near_copy(c).start()

    for p in range(n // 2):
        o = dot(fy, jnp.concatenate([own[2 * p], own[2 * p + 1]], axis=1))
        for g in range(3):
            fa[g, p * 16 : (p + 1) * 16, :] = jnp.concatenate(
                [o[g * 8 : g * 8 + 8, :LANES], o[g * 8 : g * 8 + 8, LANES:]], axis=0
            ).astype(BF)
    o = dot(fsecond[0][:, :n8], jnp.concatenate([fa[g] for g in range(3)], axis=1))
    o = jnp.concatenate([o, jnp.zeros(((3 * deep - n) * 8, 3 * LANES), F32)], axis=0).astype(BF)
    d8 = deep * 8
    for g in range(3):
        s = dot_t(
            jnp.concatenate(
                [o[t * d8 : (t + 1) * d8, g * LANES : (g + 1) * LANES] for t in range(3)], axis=1
            ),
            fz3,
        )
        part[:, g * 8 : (g + 1) * 8, :] = s.reshape(deep, 8, LANES).astype(BF)
    mate_copy(0).start()

    fetch[2].wait()
    cats(fine_blk, pad, n, terms)
    build_first(pad, first, terms)
    build_second(first[...], second, wide, terms, n)
    first[...] = dot(first[...], perm).astype(BF)

    mate_copy(0).wait_recv()
    half[:, :n, :] = (part[:, :n, :].astype(F32) + got[0, :, :n, :].astype(F32)).astype(BF)
    mate_copy(1).start()

    build_third(pad, lines, third, terms, boxes, n, None)
    first_pass(own, ROW, first, a.at[3], n, terms * 3)
    second_pass([a.at[3]], second, mid, n, terms, LANES)

    fetch[3].wait()
    cats(coarse_blk, pad, n, terms)
    build_first(pad, first_c, terms)
    r, c = grid2(4 * ROW, 4 * ROW)
    same = lax.div(r, ROW) == lax.div(c, ROW)
    rows4 = one(lax.rem(grid2(4 * ROW, PAD)[0], ROW) == grid2(4 * ROW, PAD)[1])
    cols4 = one(lax.rem(grid2(PAD, 4 * ROW)[1], ROW) == grid2(PAD, 4 * ROW)[0])

    def quad(mat):
        return jnp.where(same, dot(rows4, dot(mat, cols4).astype(BF)), 0.0).astype(BF)

    build_second(grown(first_c, quad(tpad[px][:, :PAD].astype(BF)), terms), second_c, wide, terms, n)
    first_c[...] = grown(first_c, quad(tpad[py][:, :PAD].astype(BF)), terms)
    build_third(pad, lines, third_c, terms, boxes // 2, n, growth(tpad, boxes // 2))

    def near_wait(c):
        @pl.when(near[c][2])
        def _():
            near_copy(back[c]).wait_recv()

    for c in (2, 3):
        near_wait(c)
        unpack(npk.at[c], ux.at[c - 2], slice(0, ROW), n, kappa)
        first_pass(ux.at[c - 2], ROW, first, a.at[c - 1], n, terms * 3)
    mate_copy(1).wait_recv()
    cpk[:, n:, :] = jnp.zeros((deep, ROW - n, LANES), BF)
    cpk[:, :n, :] = (half[:, :n, :].astype(F32) + got[1, :, :n, :].astype(F32)).astype(BF)
    for c in range(4):

        @pl.when(far[c][2])
        def _():
            far_copy(c).start()

    u[:, :ROW, :] = own[...]
    for c in (0, 1):
        near_wait(c)
        unpack(npk.at[c], u, slice((c + 1) * ROW, (c + 2) * ROW), n, kappa)
    first_pass(u, 3 * ROW, first, a.at[0], n, terms * 3)
    second_pass([a.at[0], a.at[1], a.at[2]], second, mid, n, terms, 0)
    acc[...] = third_pass(mid, third, terms)

    unpack_parent(cpk, cu, slice(0, ROW), n, half_k, True)
    for c in range(4):

        @pl.when(far[c][2])
        def _():
            far_copy(back[c]).wait_recv()

        if c < 2:
            unpack_parent(ppk.at[c], cu, slice((c + 1) * ROW, (c + 2) * ROW), n, half_k, False)
        else:
            unpack_parent(ppk.at[c], cx.at[c - 2], slice(0, ROW), n, half_k, False)
    first_pass(cx.at[0], ROW, first_c, a.at[1], n, terms * 3)
    first_pass(cx.at[1], ROW, first_c, a.at[2], n, terms * 3)
    first_pass(cu, 3 * ROW, first_c, a.at[0], n, terms * 3)
    second_pass([a.at[0], a.at[1], a.at[2]], second_c, mid_c, n, terms, 0)
    acc[...] += third_pass(mid_c, third_c, terms)
    flatten(lambda g, i: acc[g * n8 + i * 8 : g * n8 + (i + 1) * 8, :], out, boxes, n)

    for c in range(2):
        mate_copy(c).wait_send()
    for c in range(4):

        @pl.when(near[c][2])
        def _():
            near_copy(c).wait_send()

        @pl.when(far[c][2])
        def _():
            far_copy(c).wait_send()


VM = pl.BlockSpec(memory_space=pltpu.VMEM)


def in_hbm(x):
    return pltpu.with_memory_space_constraint(x, pltpu.HBM)


def shards(nx, ny, fine_source, fine_blocks, coarse_blocks, filters):
    boxes = fine_source.shape[2]
    terms, n = fine_blocks.shape[1], fine_blocks.shape[2]
    n8 = n * 8
    deep = (n + 2) // 3
    dma = pltpu.SemaphoreType.DMA

    def bf(*shape):
        return pltpu.VMEM(shape, BF)

    def f32(*shape):
        return pltpu.VMEM(shape, F32)

    return pl.pallas_call(
        functools.partial(kernel, boxes=boxes, nx=nx, ny=ny),
        out_shape=jax.ShapeDtypeStruct(fine_source.shape, F32),
        in_specs=[pl.BlockSpec(memory_space=pltpu.HBM)] * 4,
        out_specs=VM,
        scratch_shapes=[
            bf(*fine_source.shape),
            bf(n, 2, n),
            bf(n, ROW, LANES),
            f32(boxes, (fine_source.shape[3] // LANES + 3) * LANES),
            bf(3 * terms, n, n),
            bf(3 * terms, n, n),
            f32(3 * n8, LANES),
            f32(3 * terms * ROW, LANES),
            bf(2 * deep, ROW, LANES),
            bf(4, 2 * deep, ROW, LANES),
            bf(n, 3 * ROW, LANES),
            bf(2, n, ROW, LANES),
            bf(deep, ROW, LANES),
            bf(deep, ROW, LANES),
            bf(2, deep, ROW, LANES),
            bf(deep, ROW, LANES),
            bf(4, deep, ROW, LANES),
            bf(n, 3 * ROW, LANES),
            bf(2, n, ROW, LANES),
            f32(2, PAD, LANES),
            f32(2, PAD, LANES),
            f32(3 * terms * ROW, LANES),
            f32(terms * ROW, 4 * LANES),
            bf(terms * ROW, LANES),
            bf(terms, n8, 4 * LANES),
            bf(LANES, terms * 2 * LANES),
            bf(terms * ROW, LANES),
            bf(terms, n8, 4 * LANES),
            bf(LANES, terms * LANES),
            bf(1, n8, 2 * LANES),
            bf(3, n8, LANES),
            bf(4, terms * 3, n8, LANES),
            bf(terms, 3 * n8, 2 * LANES),
            bf(terms, 3 * n8, LANES),
            dma((4,)),
            dma((4,)),
            dma((2,)),
            dma((2,)),
            dma((4,)),
            dma((4,)),
            dma((4,)),
        ],
        compiler_params=pltpu.CompilerParams(
            vmem_limit_bytes=32 * 1024 * 1024, collective_id=0, has_side_effects=True
        ),
    )(
        in_hbm(fine_source),
        in_hbm(fine_blocks.reshape(3 * terms, n, n)),
        in_hbm(coarse_blocks.reshape(3 * terms, n, n)),
        in_hbm(filters.transpose(1, 0, 2)),
    )


def solution(mesh):
    in_specs = (P("gx", "gy", None, None), P(), P(), P())
    out_specs = P("gx", "gy", None, None)
    body = functools.partial(shards, mesh.shape["gx"], mesh.shape["gy"])
    return jax.shard_map(body, mesh=mesh, in_specs=in_specs, out_specs=out_specs, check_vma=False)
```

```python
import functools

import jax
import jax.numpy as jnp
from jax import lax
from jax.experimental import pallas as pl
from jax.experimental.pallas import tpu as pltpu
from jax.sharding import PartitionSpec as P

BF = jnp.bfloat16
F32 = jnp.float32
MESH = pl.DeviceIdType.MESH
ROW = 24
PAD = 32
LANES = 128


def dot(a, b):
    return jnp.dot(a, b, preferred_element_type=F32)


def dot_t(a, b):
    return lax.dot_general(a, b, (((1,), (1,)), ((), ())), preferred_element_type=F32)


def grid2(rows, cols):
    r = lax.broadcasted_iota(jnp.int32, (rows, cols), 0)
    c = lax.broadcasted_iota(jnp.int32, (rows, cols), 1)
    return r, c


def one(cond):
    return jnp.where(cond, 1.0, 0.0).astype(BF)


def repeat_lanes(rows, period, valid):
    r, c = grid2(rows, LANES)
    return one((lax.rem(c, period) == r) & (c < valid))


def repeat_rows(cols, period, valid):
    r, c = grid2(LANES, cols)
    return one((lax.rem(r, period) == c) & (r < valid))


def cats(blk, pad, n, terms):
    pad[...] = jnp.zeros_like(pad)
    for p in range(3 * terms):
        pad[p * ROW : p * ROW + n, :n] = blk[p].astype(F32)


def three(pad, m, terms):
    return [pad[(e * terms + m) * ROW : (e * terms + m + 1) * ROW, :] for e in range(3)]


def build_first(pad, first, terms):
    for m in range(terms):
        low, mid, up = three(pad, m, terms)
        first[m * ROW : (m + 1) * ROW, :] = (
            mid + pltpu.roll(up, ROW, 1) + pltpu.roll(low, 2 * ROW, 1)
        ).astype(BF)


def grown(first, mat, terms):
    step = mat.shape[0]
    rows = [dot(mat, first[m : m + step, :]).astype(BF) for m in range(0, terms * ROW, step)]
    return jnp.concatenate(rows, axis=0)


def widen(source, spread, wide, out, n, count, lanes):
    wide[: source.shape[0], :lanes] = dot(source, spread)
    r, c = grid2(16, lanes)
    keep = lax.rem(c, 8) == lax.rem(r, 8)

    def body(m, carry):
        base = pl.multiple_of(m * ROW, 8)
        block = wide[pl.ds(base, ROW), :lanes]
        for i in range(0, n, 2):
            pair = jnp.concatenate(
                [jnp.broadcast_to(block[i + h : i + h + 1, :], (8, lanes)) for h in range(2)], axis=0
            )
            out[m, i * 8 : (i + 2) * 8, :lanes] = jnp.where(keep, pair, 0.0).astype(BF)
        return carry

    if count == 1:
        body(0, 0)
    else:
        lax.fori_loop(0, count, body, 0, unroll=2)


def spread_eight(n, lanes, groups):
    r, c = grid2(LANES, lanes)
    n8 = n * 8
    return one((r == lax.div(c, n8) * ROW + lax.div(lax.rem(c, n8), 8)) & (c < groups * n8))


def build_second(source, second, wide, terms, n):
    widen(source, spread_eight(n, 4 * LANES, 3), wide, second, n, terms, 4 * LANES)


def build_third(pad, lines, third, terms, boxes, n, grow):
    both = grow is not None
    lines[...] = dot(pad[:, :PAD].astype(BF), repeat_lanes(PAD, n, boxes * n * (3 if both else 1)))
    col = lax.div(grid2(ROW, LANES)[1], n)
    spare = jnp.zeros((LANES - boxes * ROW, LANES), F32)
    for m in range(terms):
        low, mid, up = three(lines, m, terms)
        main, other = [], []
        for z in range(boxes):
            shift = boxes if both else 0
            side = jnp.where(col == shift + z + 1, up, 0.0) if z + 1 < boxes else jnp.zeros_like(up)
            if z > 0:
                side = jnp.where(col == shift + z - 1, low, side)
            if both:
                main.append(jnp.where((col == z) | (col == 2 * boxes + z), mid, side))
            else:
                main.append(jnp.where(col == z, mid, 0.0))
                other.append(side)
        if both:
            tile = jnp.concatenate(main, axis=0).astype(BF)
            third[:, m * LANES : (m + 1) * LANES] = dot(grow, tile).astype(BF)
        else:
            at = m * 2 * LANES
            third[:, at : at + LANES] = jnp.concatenate(main + [spare], axis=0).astype(BF)
            third[:, at + LANES : at + 2 * LANES] = jnp.concatenate(other + [spare], axis=0).astype(BF)


def growth(tpad, boxes):
    rows = [
        tpad[e][:ROW] if z == 0 else pltpu.roll(tpad[e][:ROW], z * ROW, 1)
        for z in range(boxes)
        for e in range(2)
    ]
    rows.append(jnp.zeros((LANES - 2 * boxes * ROW, LANES), F32))
    return jnp.concatenate(rows, axis=0).astype(BF)[:, : boxes * ROW]


def pair_mats(mats, boxes_in, boxes_out, n):
    r, c = grid2(LANES, LANES)
    row, col = lax.div(r, n), lax.div(c, n)
    fine, parent = (col, row) if boxes_in > boxes_out else (row, col)
    keep = (lax.div(fine, 2) == parent) & (r < boxes_out * n) & (c < boxes_in * n)
    left = repeat_rows(PAD, n, boxes_out * n)
    right = repeat_lanes(PAD, n, boxes_in * n)
    tiles = [dot(left, dot(mats[e], right).astype(BF)) for e in range(2)]
    return jnp.where(keep, jnp.where(lax.rem(fine, 2) == 0, tiles[0], tiles[1]), 0.0)


def lane(shape):
    return lax.broadcasted_iota(jnp.int32, shape, 1)


def pack(src, dst, n, kappa):
    at = lane((ROW, LANES))
    for q in range((n + 2) // 3):
        tile = [src[3 * q + h].astype(F32) if 3 * q + h < n else None for h in range(3)]
        r1 = pltpu.roll(tile[1], kappa, 1)
        dst[2 * q] = jnp.where(at < kappa, tile[0], r1).astype(BF)
        r2 = jnp.zeros_like(r1) if tile[2] is None else pltpu.roll(tile[2], 2 * kappa - LANES, 1)
        dst[2 * q + 1] = jnp.where(at < 2 * kappa - LANES, r1, r2).astype(BF)


def unpack(src, dst, rows, n, kappa):
    at = lane((ROW, LANES))
    for q in range((n + 2) // 3):
        a, b = src[2 * q].astype(F32), src[2 * q + 1].astype(F32)
        dst[3 * q, rows, :] = a.astype(BF)
        dst[3 * q + 1, rows, :] = pltpu.roll(jnp.where(at >= kappa, a, b), LANES - kappa, 1).astype(BF)
        if 3 * q + 2 < n:
            dst[3 * q + 2, rows, :] = pltpu.roll(b, 2 * (LANES - kappa), 1).astype(BF)


def unpack_parent(src, dst, rows, n, kappa, twice):
    at = lane((ROW, LANES))
    deep = (n + 2) // 3
    for s in range(deep):
        tile = src[s].astype(F32)
        for t in range(3):
            if t * deep + s < n:
                v = tile if t == 0 else pltpu.roll(tile, LANES - t * kappa, 1)
                other = 0.0
                if twice:
                    other = tile if t == 1 else pltpu.roll(tile, (LANES - (t - 1) * kappa) % LANES, 1)
                if twice:
                    other = jnp.where(at < 2 * kappa, other, 0.0)
                dst[t * deep + s, rows, :] = jnp.where(at < kappa, v, other).astype(BF)


def unpack_sides(plus, minus, dst, n, kappa):
    at = lane((ROW, LANES))
    deep = (n + 2) // 3
    for s in range(deep):
        up, low = plus[s].astype(F32), minus[s].astype(F32)
        for t in range(3):
            if t * deep + s < n:
                v = up if t == 0 else pltpu.roll(up, LANES - t * kappa, 1)
                w = low if t == 2 else pltpu.roll(low, (2 - t) * kappa, 1)
                w = jnp.where((at >= 2 * kappa) & (at < 3 * kappa), w, 0.0)
                dst[t * deep + s] = jnp.where(at < kappa, v, w).astype(BF)


def tiles_of(base, rows, n):
    return base // LANES, (base + rows * n - 1) // LANES


def mirror(n):
    r, c = grid2(LANES, LANES)
    group, p = lax.div(c, ROW), lax.rem(c, ROW)
    g, s = lax.div(p, 8), lax.rem(p, 8)
    count = jnp.minimum(n - 8 * g, 8)
    return one((s < count) & (r == group * ROW + 8 * g + count - 1 - s) & (group < 3))


def skew(v, n):
    v = pltpu.roll(v, 0, 1, stride=n // 2, stride_axis=0)
    return pltpu.roll(v, 0, 1, stride=n - n // 2, stride_axis=0)


def unflatten(raw, flat, own, boxes, n):
    size = raw.shape[-1]
    flat[:, size // LANES * LANES :] = jnp.zeros((boxes, flat.shape[1] - size // LANES * LANES), F32)
    flat[:, :size] = raw[0, 0].astype(F32)
    s, at = grid2(8, LANES)
    offset = at + s * n
    place = lax.rem(at + s * n, LANES)
    below = [place < (z + 1) * n for z in range(boxes)]
    for i in range(n):
        rows = []
        for g in range(ROW // 8):
            base = (i * n + 8 * g + min(8, n - 8 * g) - 1) * n
            t = (base - 7 * n) // LANES
            c = base - t * LANES
            v = None
            for z in reversed(range(boxes)):

                def tile(k):
                    line = flat[z : z + 1, (t + k) * LANES : (t + k + 1) * LANES]
                    return jnp.broadcast_to(line, (8, LANES))

                w = jnp.where(offset >= c, tile(0), tile(1))
                if c + n > 2 * LANES:
                    w = jnp.where(offset >= c - LANES, w, tile(2))
                w = pltpu.roll(w, (z * n - c) % LANES, 1)
                v = w if v is None else jnp.where(below[z], w, v)
            rows.append(skew(v, n))
        own[i] = jnp.concatenate(rows, axis=0).astype(BF)


def flatten(rows, out, boxes, n):
    size = out.shape[-1]
    s, at = grid2(8, LANES)
    offset = at - s * n
    total = [[None] * (-(-size // LANES)) for _ in range(boxes)]
    for i in range(n):
        for g in range(ROW // 8):
            base = (i * n + 8 * g) * n
            count = min(8, n - 8 * g)
            first, last = base // LANES, (base + count * n - 1) // LANES
            c = base - first * LANES
            v = skew(rows(g, i), n)
            turned = [pltpu.roll(v, (c - z * ROW) % LANES, 1) for z in range(boxes)]
            for t in range(first, last + 1):
                lo = c - (t - first) * LANES
                keep = (offset >= lo) & (offset < lo + n)
                if count < 8:
                    keep = keep & (s < count)
                for z in range(boxes):
                    old = total[z][t]
                    total[z][t] = jnp.where(keep, turned[z], 0.0 if old is None else old)
        for t in range(len(total[0])):
            if total[0][t] is not None and ((t + 1) * LANES <= (i + 1) * n * n or i == n - 1):
                end = min((t + 1) * LANES, size)
                for z in range(boxes):
                    line = jnp.sum(total[z][t], axis=0, keepdims=True)
                    out[0, 0, z : z + 1, t * LANES : end] = line[:, : end - t * LANES]
                    total[z][t] = None


def first_pass(u, rows, w, a, n, blocks):
    def body(p, carry):
        rhs = jnp.concatenate([u[2 * p, :rows, :], u[2 * p + 1, :rows, :]], axis=1)
        o = dot(w[:, :rows], rhs)
        at = pl.multiple_of(p * 16, 16)
        for t in range(blocks):
            a[t, pl.ds(at, 16), :] = jnp.concatenate(
                [o[t * 8 : t * 8 + 8, :LANES], o[t * 8 : t * 8 + 8, LANES:]], axis=0
            ).astype(BF)
        return carry

    lax.fori_loop(0, n // 2, body, 0, unroll=True)


def first_pass_sides(u, w, a_up, a_low, n, blocks, kappa):
    at = lane((16, LANES))
    for p in range(n // 2):
        o = dot(w[:, :ROW], jnp.concatenate([u[2 * p], u[2 * p + 1]], axis=1))
        rows = slice(p * 16, (p + 1) * 16)
        for t in range(blocks):
            v = jnp.concatenate([o[t * 8 : t * 8 + 8, :LANES], o[t * 8 : t * 8 + 8, LANES:]], axis=0)
            a_up[t, rows, :] = jnp.where(at < kappa, v, 0.0).astype(BF)
            a_low[t, rows, :] = jnp.where(at < kappa, 0.0, v).astype(BF)


def second_pass(fields, second, mid, n, terms, at):
    n8 = n * 8
    k = len(fields) * n8

    def body(m, carry):
        rhs = jnp.concatenate(
            [jnp.concatenate([a[m * 3 + g] for g in range(3)], axis=1) for a in fields], axis=0
        )
        p = dot(second[m][:, :k], rhs).astype(BF)
        for g in range(3):
            mid[m, g * n8 : (g + 1) * n8, at : at + LANES] = p[:, g * LANES : (g + 1) * LANES]
        return carry

    lax.fori_loop(0, terms, body, 0, unroll=True)


def third_pass(mid, third, terms):
    return dot_t(jnp.concatenate([mid[m] for m in range(terms)], axis=1), third[...])


def kernel(
    raw_hbm,
    fine_hbm,
    coarse_hbm,
    filt_hbm,
    out,
    raw,
    filt,
    own,
    flat,
    fine_blk,
    coarse_blk,
    acc,
    lines,
    opk,
    npk,
    u,
    ux,
    part,
    half,
    got,
    cpk,
    ppk,
    cu,
    cx,
    fpad,
    tpad,
    pad,
    wide,
    first,
    second,
    third,
    first_c,
    second_c,
    third_c,
    fsecond,
    fa,
    a,
    mid,
    mid_c,
    fsend,
    frecv,
    psend,
    precv,
    csend,
    crecv,
    bsem,
    *,
    boxes,
    nx,
    ny,
):
    n = own.shape[0]
    n8 = n * 8
    terms = fine_blk.shape[0] // 3
    kappa = boxes * n
    half_k = kappa // 2
    deep = (n + 2) // 3
    x, y = lax.axis_index("gx"), lax.axis_index("gy")
    px, py = lax.rem(x, 2), lax.rem(y, 2)
    mates = [(x + 1 - 2 * px, y), (x, y + 1 - 2 * py)]
    near = [(x, y + 1, y < ny - 1), (x, y - 1, y > 0), (x + 1, y, x < nx - 1), (x - 1, y, x > 0)]
    far = [(x, y + 2, y < ny - 2), (x, y - 2, y > 1), (x + 2, y, x < nx - 2), (x - 2, y, x > 1)]
    back = [1, 0, 3, 2]

    def near_copy(c):
        b = back[c]
        return pltpu.make_async_remote_copy(
            src_ref=opk.at[:, :n, :],
            dst_ref=npk.at[b, :, :n, :],
            send_sem=fsend.at[c],
            recv_sem=frecv.at[b],
            device_id=near[c][:2],
            device_id_type=MESH,
        )

    def far_copy(c):
        b = back[c]
        return pltpu.make_async_remote_copy(
            src_ref=cpk.at[:, :n, :],
            dst_ref=ppk.at[b, :, :n, :],
            send_sem=csend.at[c],
            recv_sem=crecv.at[b],
            device_id=far[c][:2],
            device_id_type=MESH,
        )

    def mate_copy(c):
        return pltpu.make_async_remote_copy(
            src_ref=(part, half)[c].at[:, :n, :],
            dst_ref=got.at[c, :, :n, :],
            send_sem=psend.at[c],
            recv_sem=precv.at[c],
            device_id=mates[c],
            device_id_type=MESH,
        )

    fetch = [
        pltpu.make_async_copy(raw_hbm, raw, bsem.at[2]),
        pltpu.make_async_copy(filt_hbm, filt, bsem.at[3]),
        pltpu.make_async_copy(fine_hbm, fine_blk, bsem.at[0]),
        pltpu.make_async_copy(coarse_hbm, coarse_blk, bsem.at[1]),
    ]
    for f in fetch:
        f.start()
    barrier = pltpu.get_barrier_semaphore()
    count = jnp.int32(0)
    for dx, dy, exists in near + far:
        count = count + jnp.where(exists, 1, 0)

        @pl.when(exists)
        def _():
            pl.semaphore_signal(barrier, inc=1, device_id=(dx, dy), device_id_type=MESH)

    for c in range(4):
        npk[c, :, n:, :] = jnp.zeros((2 * deep, ROW - n, LANES), BF)
        ppk[c, :, n:, :] = jnp.zeros((deep, ROW - n, LANES), BF)

        @pl.when(jnp.logical_not(near[c][2]))
        def _():
            npk[c, :, :n, :] = jnp.zeros((2 * deep, n, LANES), BF)

        @pl.when(jnp.logical_not(far[c][2]))
        def _():
            ppk[c, :, :n, :] = jnp.zeros((deep, n, LANES), BF)

    fetch[0].wait()
    fetch[1].wait()
    unflatten(raw, flat, own, boxes, n)
    pack(own, opk, n, kappa)

    fpad[...] = jnp.zeros_like(fpad)
    for e in range(2):
        fpad[e, :n, :n] = filt[:, e, :].astype(F32)
    r, c = grid2(PAD, PAD)
    eye = one(r == c)
    mats = [fpad[e][:, :PAD].astype(BF) for e in range(2)]
    tpad[...] = jnp.zeros_like(tpad)
    for e in range(2):
        tpad[e, :, :PAD] = dot_t(eye, mats[e])
    perm = mirror(n)
    fy = dot(fpad[py][:ROW, :].astype(BF), perm)[:, :ROW].astype(BF)
    fx = fpad[px][:ROW, :].astype(BF)
    widen(fx, spread_eight(n, 2 * LANES, 1), wide, fsecond, n, 1, 2 * LANES)
    fz = pair_mats(mats, boxes, boxes // 2, n)
    turns = [fz if t == 0 else pltpu.roll(fz, t * half_k, 0) for t in range(3)]
    fz3 = jnp.concatenate(turns, axis=1).astype(BF)

    pl.semaphore_wait(barrier, count)
    for c in (2, 3, 0, 1):

        @pl.when(near[c][2])
        def _():
            near_copy(c).start()

    for p in range(n // 2):
        o = dot(fy, jnp.concatenate([own[2 * p], own[2 * p + 1]], axis=1))
        for g in range(3):
            fa[g, p * 16 : (p + 1) * 16, :] = jnp.concatenate(
                [o[g * 8 : g * 8 + 8, :LANES], o[g * 8 : g * 8 + 8, LANES:]], axis=0
            ).astype(BF)
    o = dot(fsecond[0][:, :n8], jnp.concatenate([fa[g] for g in range(3)], axis=1))
    o = jnp.concatenate([o, jnp.zeros(((3 * deep - n) * 8, 3 * LANES), F32)], axis=0).astype(BF)
    d8 = deep * 8
    for g in range(3):
        s = dot_t(
            jnp.concatenate(
                [o[t * d8 : (t + 1) * d8, g * LANES : (g + 1) * LANES] for t in range(3)], axis=1
            ),
            fz3,
        )
        part[:, g * 8 : (g + 1) * 8, :] = s.reshape(deep, 8, LANES).astype(BF)
    mate_copy(0).start()

    fetch[2].wait()
    cats(fine_blk, pad, n, terms)
    build_first(pad, first, terms)
    build_second(first[...], second, wide, terms, n)
    first[...] = dot(first[...], perm).astype(BF)

    mate_copy(0).wait_recv()
    half[:, :n, :] = (part[:, :n, :].astype(F32) + got[0, :, :n, :].astype(F32)).astype(BF)
    mate_copy(1).start()

    build_third(pad, lines, third, terms, boxes, n, None)
    first_pass(own, ROW, first, a.at[3], n, terms * 3)
    second_pass([a.at[3]], second, mid, n, terms, LANES)

    fetch[3].wait()
    cats(coarse_blk, pad, n, terms)
    build_first(pad, first_c, terms)
    r, c = grid2(4 * ROW, 4 * ROW)
    same = lax.div(r, ROW) == lax.div(c, ROW)
    rows4 = one(lax.rem(grid2(4 * ROW, PAD)[0], ROW) == grid2(4 * ROW, PAD)[1])
    cols4 = one(lax.rem(grid2(PAD, 4 * ROW)[1], ROW) == grid2(PAD, 4 * ROW)[0])

    def quad(mat):
        return jnp.where(same, dot(rows4, dot(mat, cols4).astype(BF)), 0.0).astype(BF)

    build_second(grown(first_c, quad(tpad[px][:, :PAD].astype(BF)), terms), second_c, wide, terms, n)
    first_c[...] = grown(first_c, quad(tpad[py][:, :PAD].astype(BF)), terms)
    build_third(pad, lines, third_c, terms, boxes // 2, n, growth(tpad, boxes // 2))

    def near_wait(c):
        @pl.when(near[c][2])
        def _():
            near_copy(back[c]).wait_recv()

    for c in (2, 3):
        near_wait(c)
        unpack(npk.at[c], ux.at[c - 2], slice(0, ROW), n, kappa)
        first_pass(ux.at[c - 2], ROW, first, a.at[c - 1], n, terms * 3)
    mate_copy(1).wait_recv()
    cpk[:, n:, :] = jnp.zeros((deep, ROW - n, LANES), BF)
    cpk[:, :n, :] = (half[:, :n, :].astype(F32) + got[1, :, :n, :].astype(F32)).astype(BF)
    for c in range(4):

        @pl.when(far[c][2])
        def _():
            far_copy(c).start()

    u[:, :ROW, :] = own[...]
    for c in (0, 1):
        near_wait(c)
        unpack(npk.at[c], u, slice((c + 1) * ROW, (c + 2) * ROW), n, kappa)
    first_pass(u, 3 * ROW, first, a.at[0], n, terms * 3)
    second_pass([a.at[0], a.at[1], a.at[2]], second, mid, n, terms, 0)
    acc[...] = third_pass(mid, third, terms)

    unpack_parent(cpk, cu, slice(0, ROW), n, half_k, True)
    for c in range(4):

        @pl.when(far[c][2])
        def _():
            far_copy(back[c]).wait_recv()

        if c < 2:
            unpack_parent(ppk.at[c], cu, slice((c + 1) * ROW, (c + 2) * ROW), n, half_k, False)
    unpack_sides(ppk.at[2], ppk.at[3], cx, n, half_k)
    first_pass_sides(cx, first_c, a.at[1], a.at[2], n, terms * 3, half_k)
    first_pass(cu, 3 * ROW, first_c, a.at[0], n, terms * 3)
    second_pass([a.at[0], a.at[1], a.at[2]], second_c, mid_c, n, terms, 0)
    acc[...] += third_pass(mid_c, third_c, terms)
    flatten(lambda g, i: acc[g * n8 + i * 8 : g * n8 + (i + 1) * 8, :], out, boxes, n)

    for c in range(2):
        mate_copy(c).wait_send()
    for c in range(4):

        @pl.when(near[c][2])
        def _():
            near_copy(c).wait_send()

        @pl.when(far[c][2])
        def _():
            far_copy(c).wait_send()


VM = pl.BlockSpec(memory_space=pltpu.VMEM)


def in_hbm(x):
    return pltpu.with_memory_space_constraint(x, pltpu.HBM)


def shards(nx, ny, fine_source, fine_blocks, coarse_blocks, filters):
    boxes = fine_source.shape[2]
    terms, n = fine_blocks.shape[1], fine_blocks.shape[2]
    n8 = n * 8
    deep = (n + 2) // 3
    dma = pltpu.SemaphoreType.DMA

    def bf(*shape):
        return pltpu.VMEM(shape, BF)

    def f32(*shape):
        return pltpu.VMEM(shape, F32)

    return pl.pallas_call(
        functools.partial(kernel, boxes=boxes, nx=nx, ny=ny),
        out_shape=jax.ShapeDtypeStruct(fine_source.shape, F32),
        in_specs=[pl.BlockSpec(memory_space=pltpu.HBM)] * 4,
        out_specs=VM,
        scratch_shapes=[
            bf(*fine_source.shape),
            bf(n, 2, n),
            bf(n, ROW, LANES),
            f32(boxes, (fine_source.shape[3] // LANES + 3) * LANES),
            bf(3 * terms, n, n),
            bf(3 * terms, n, n),
            f32(3 * n8, LANES),
            f32(3 * terms * ROW, LANES),
            bf(2 * deep, ROW, LANES),
            bf(4, 2 * deep, ROW, LANES),
            bf(n, 3 * ROW, LANES),
            bf(2, n, ROW, LANES),
            bf(deep, ROW, LANES),
            bf(deep, ROW, LANES),
            bf(2, deep, ROW, LANES),
            bf(deep, ROW, LANES),
            bf(4, deep, ROW, LANES),
            bf(n, 3 * ROW, LANES),
            bf(n, ROW, LANES),
            f32(2, PAD, LANES),
            f32(2, PAD, LANES),
            f32(3 * terms * ROW, LANES),
            f32(terms * ROW, 4 * LANES),
            bf(terms * ROW, LANES),
            bf(terms, n8, 4 * LANES),
            bf(LANES, terms * 2 * LANES),
            bf(terms * ROW, LANES),
            bf(terms, n8, 4 * LANES),
            bf(LANES, terms * LANES),
            bf(1, n8, 2 * LANES),
            bf(3, n8, LANES),
            bf(4, terms * 3, n8, LANES),
            bf(terms, 3 * n8, 2 * LANES),
            bf(terms, 3 * n8, LANES),
            dma((4,)),
            dma((4,)),
            dma((2,)),
            dma((2,)),
            dma((4,)),
            dma((4,)),
            dma((4,)),
        ],
        compiler_params=pltpu.CompilerParams(
            vmem_limit_bytes=32 * 1024 * 1024, collective_id=0, has_side_effects=True
        ),
    )(
        in_hbm(fine_source),
        in_hbm(fine_blocks.reshape(3 * terms, n, n)),
        in_hbm(coarse_blocks.reshape(3 * terms, n, n)),
        in_hbm(filters.transpose(1, 0, 2)),
    )


def solution(mesh):
    in_specs = (P("gx", "gy", None, None), P(), P(), P())
    out_specs = P("gx", "gy", None, None)
    body = functools.partial(shards, mesh.shape["gx"], mesh.shape["gy"])
    return jax.shard_map(body, mesh=mesh, in_specs=in_specs, out_specs=out_specs, check_vma=False)
```
